32 devices in a mesh: stack: 2 (over y), date: 4 (over x, core), line: 4 (over z).
Axes of the slice: x: 2, y: 2, z: 4, core: 2. Of those that a mesh axis runs over, the one named last changes fastest.
Arguments:
- slc: float32 [4, 2, 512, 1280], P('date', None, 'stack', 'line'), parts along dimension 2, may hold values from -6 to 6
- band_start: int32 [4], replicated, may hold values from 0 to 640, as said below
- band_stop: int32 [4], replicated, may hold values from 640 to 1280, as said below
Outputs:
- interferogram: float32 [4, 2, 512, 256], P('date', None, 'stack', 'line'), parts along dimension 2
The draws below stay inside these ranges and needn't reach their ends.
There are 2 independent parts, one for each index of `stack`. The reference program is written for one: setup_inputs(seed, part) draws one part's arguments, and reference() takes and returns one part's arrays. A program takes and returns all parts, laid end to end along the dimension named above; an argument that names none is the same for every part. Nothing has to cross between parts.
Inputs may be any that keep to these rules, and one draw needn't show every extreme that they name: For every pair, band_stop - band_start lies between 640 and 960; at least one pair keeps exactly 960 bins, and some pair keeps exactly 640 bins ending at 1280. `band_stop`: see band_start.
All inputs are finite; a program needn't handle non-finite values.
Results may differ from the reference program's by a relative error of at most 0.0001.
Values sent between devices are 32-bit elements; how exact they have to be, the bound alone decides.
A program may use at most 64 MiB of HBM per device.

```python
import jax
import jax.numpy as jnp

COLS = 256
LOOKS = 5
LINES = 1280
DATES = 4


def band_pair(key):
    key_width = jax.random.fold_in(key, 11)
    key_chosen = jax.random.fold_in(key, 23)
    key_offset = jax.random.fold_in(key, 37)
    narrowest = LINES // 2
    widest = 3 * LINES // 4
    order = jax.random.permutation(key_chosen, jnp.arange(DATES, dtype=jnp.int32))
    pair_ids = jnp.arange(DATES, dtype=jnp.int32)
    widths = jax.random.randint(key_width, (DATES,), narrowest, widest + 1)
    widths = jnp.where(pair_ids == order[0], widest, widths)
    widths = jnp.where((pair_ids == order[1]) | (pair_ids == order[2]), narrowest, widths)
    starts = jax.random.randint(key_offset, (DATES,), 0, LINES - widths + 1)
    starts = jnp.where(pair_ids == order[1], LINES - narrowest, starts)
    starts = jnp.where(pair_ids == order[2], 0, starts)
    return (starts.astype(jnp.int32), (starts + widths).astype(jnp.int32))


def draw_band_start(key, part):
    return band_pair(key)[0]


def draw_band_stop(key, part):
    return band_pair(key)[1]


def steps_of(own_key, shape, split, least, largest):
    factor_of, own = 1.0, jax.random.fold_in(own_key, 6)
    for dim, parts in split:
        steps = jnp.exp(jax.random.uniform(jax.random.fold_in(own, dim), (parts,), jnp.float32, least / len(split), largest / len(split)))
        factor_of = factor_of * jnp.repeat(steps, shape[dim] // parts).reshape([-1 if axis == dim else 1 for axis in range(len(shape))])
    return factor_of


def normal_values(key, dims, width, bound, pieces=(), kind=jnp.bfloat16):
    gain = steps_of(key, dims, pieces, -0.22, 0.18) if pieces else 1.0
    drawn = jax.random.normal(key, dims, jnp.float32) * width * gain
    return jnp.minimum(jnp.maximum(drawn, -bound), bound).astype(kind)


def setup_inputs(seed: int = 0, part: int = 0) -> dict:
    key_of = jax.random.split(jax.random.key(seed), 4)
    part_splits = jax.random.split(jax.random.fold_in(key_of[3], part), 4)
    return {
        "slc": normal_values(part_splits[0], (DATES, 2, COLS, LINES), 1.0, 6.0, ((0, 4), (3, 4)), jnp.float32),
        "band_start": draw_band_start(jax.random.fold_in(key_of[3], 71), part),
        "band_stop": draw_band_stop(jax.random.fold_in(key_of[3], 71), part),
    }


def reference(slc, band_start, band_stop):
    images = slc[:, 0] + 1j * slc[:, 1]
    spectra = jnp.fft.fft(images, axis=-1)
    partner = jnp.roll(spectra, -1, axis=0)
    bins_all = jnp.arange(LINES, dtype=jnp.int32)
    keep_mask = (bins_all[None, :] >= band_start[:, None]) & (bins_all[None, :] < band_stop[:, None])
    keep_mask = keep_mask[:, None, :]
    ref_signal = jnp.fft.ifft(jnp.where(keep_mask, spectra, 0), axis=-1)
    sec_signal = jnp.fft.ifft(jnp.where(keep_mask, partner, 0), axis=-1)
    product = ref_signal * jnp.conj(sec_signal)
    looked = product.reshape(DATES, COLS, LINES // LOOKS, LOOKS).mean(axis=-1)
    return jnp.stack([jnp.real(looked), jnp.imag(looked)], axis=1).astype(jnp.float32)
```

```python
import functools

import jax
import jax.numpy as jnp
import numpy as np
from jax import lax
from jax.experimental import pallas as pl
from jax.experimental.pallas import tpu as pltpu
from jax.sharding import PartitionSpec as P

LOOKS = 5
LANES = 128
MESH = pl.DeviceIdType.MESH
CHUNK = 16
SMALL = 16


def layout(width):
    full = width // LANES * LANES
    tail = width - full
    assert 2 * tail in (0, LANES)
    comp = np.concatenate([np.zeros(full), np.ones(full), np.zeros(tail), np.ones(tail)])
    index = np.concatenate([np.arange(full), np.arange(full), np.arange(tail) + full, np.arange(tail) + full])
    return full, tail, comp.astype(np.int64), index.astype(np.int64)


def split(values):
    high = values.astype(jnp.bfloat16)
    return high, (values - high.astype(jnp.float32)).astype(jnp.bfloat16)


def tables(outer, width):
    full, tail, comp, index = layout(width)
    angle = 2.0 * np.pi / width * (index[:, None] * index[None, :] % width)
    c, s = np.cos(angle), np.sin(angle)
    same = comp[:, None] == comp[None, :]
    to_re = (comp[:, None] == 1) & (comp[None, :] == 0)
    dense = np.where(same, c, np.where(to_re, s, -s)).astype(np.float32)
    high = dense.astype(jnp.bfloat16)
    low = (dense - high.astype(np.float32)).astype(jnp.bfloat16)
    inner = np.stack([high, low])
    lines = outer * width
    turn = 2.0 * np.pi / lines * (np.arange(outer)[:, None] * index[None, :] % lines)
    along = np.cos(turn)
    across = np.where(comp[None, :] == 0, np.sin(turn), -np.sin(turn))
    twist = np.stack([along, across], axis=1).astype(np.float32)
    bins = (np.arange(outer)[:, None] + outer * index[None, :]).astype(np.int32)[:, None, :]
    samples = width // LOOKS
    target = index // LOOKS + samples * comp
    pool = (target[:, None] == np.arange(2 * samples)[None, :]).astype(jnp.bfloat16)
    return inner, twist, bins, pool


def chunk_sizes(columns):
    sizes, left = [], columns
    while left > CHUNK and left % SMALL == 0:
        sizes.append(CHUNK)
        left -= CHUNK
    if left % SMALL == 0:
        return sizes + [SMALL] * (left // SMALL)
    return sizes + [left]


class Row:
    def __init__(self, re, im, tail):
        self.re, self.im, self.tail = re, im, tail

    def __add__(self, other):
        return Row(self.re + other.re, self.im + other.im, None if self.tail is None else self.tail + other.tail)

    def __sub__(self, other):
        return Row(self.re - other.re, self.im - other.im, None if self.tail is None else self.tail - other.tail)

    def flat(self):
        parts = [self.re, self.im] + ([] if self.tail is None else [self.tail])
        return jnp.concatenate(parts, axis=-1)


def as_row(values, full, tail):
    return Row(
        values[:, :full],
        values[:, full : 2 * full],
        values[:, 2 * full :] if tail else None,
    )


def swapped(tail_values):
    return pltpu.roll(tail_values, LANES // 2, 1)


def first_half(tail_values):
    return lax.broadcasted_iota(jnp.int32, tail_values.shape, 1) < LANES // 2


def times_minus_i(row):
    tail = row.tail
    if tail is not None:
        turned = swapped(tail)
        tail = jnp.where(first_half(tail), turned, -turned)
    return Row(row.im, -row.re, tail)


def times_phase(row, c, s):
    tail = row.tail
    if tail is not None:
        turned = swapped(tail) * s
        tail = tail * c + jnp.where(first_half(tail), turned, -turned)
    return Row(row.re * c + row.im * s, row.im * c - row.re * s, tail)


def short_dft(rows):
    count = len(rows)
    if count == 1:
        return rows
    if count % 2:
        result = []
        for k in range(count):
            total = rows[0]
            for n in range(1, count):
                angle = 2.0 * np.pi * (n * k % count) / count
                total = total + times_phase(rows[n], float(np.cos(angle)), float(np.sin(angle)))
            result.append(total)
        return result
    even, odd = short_dft(rows[0::2]), short_dft(rows[1::2])
    half = count // 2
    low, high = [], []
    for k in range(half):
        if k == 0:
            turned = odd[k]
        elif 4 * k == count:
            turned = times_minus_i(odd[k])
        else:
            angle = 2.0 * np.pi * k / count
            turned = times_phase(odd[k], float(np.cos(angle)), float(np.sin(angle)))
        low.append(even[k] + turned)
        high.append(even[k] - turned)
    return low + high


def twisted(row, twist, full, tail):
    along, across = twist[0:1, :], twist[1:2, :]
    tail_values = row.tail
    if tail_values is not None:
        tail_values = tail_values * along[:, 2 * full :] + swapped(tail_values) * across[:, 2 * full :]
    return Row(
        row.re * along[:, :full] + row.im * across[:, :full],
        row.im * along[:, :full] + row.re * across[:, full : 2 * full],
        tail_values,
    )


def times_conj(ref, sec):
    tail = None
    if ref.tail is not None:
        straight = ref.tail * sec.tail
        crossed = ref.tail * swapped(sec.tail)
        tail = jnp.where(
            first_half(straight), straight + swapped(straight), crossed - swapped(crossed)
        )
    return Row(
        ref.re * sec.re + ref.im * sec.im,
        ref.im * sec.re - ref.re * sec.im,
        tail,
    )


def kernel(
    slc_ref, inner_hbm, twist_hbm, bins_hbm, pool_hbm, start_hbm, stop_hbm, out_ref,
    raw, packed, inner, twist_ref, bins_ref, pool_ref, start_ref, stop_ref, gathered, spectrum, partner, looked, landed,
    load_sem, table_sem, in_send, in_recv, date_send, date_recv, out_send, out_recv,
):
    outer = lax.axis_size("line")
    dates = lax.axis_size("date")
    me = lax.axis_index("line")
    date = lax.axis_index("date")
    width, columns_all = raw.shape[1], raw.shape[2]
    columns = columns_all // outer
    sizes = chunk_sizes(columns)
    chunks = len(sizes)
    begins = [sum(sizes[:i]) for i in range(chunks)]
    full, tail, _, _ = layout(width)
    previous = lax.rem(date + dates - 1, dates)
    following = lax.rem(date + 1, dates)

    barrier = pltpu.get_barrier_semaphore()
    for step in range(1, outer):
        pl.semaphore_signal(
            barrier, inc=1, device_id={"line": lax.rem(me + step, outer)}, device_id_type=MESH
        )
    for other in (previous, following):
        pl.semaphore_signal(barrier, inc=1, device_id={"date": other}, device_id_type=MESH)

    load = pltpu.make_async_copy(slc_ref.at[0], raw, load_sem)
    load.start()
    tables_in = [
        pltpu.make_async_copy(source, target, table_sem.at[t])
        for t, (source, target) in enumerate(
            [
                (start_hbm, start_ref),
                (stop_hbm, stop_ref),
                (twist_hbm, twist_ref),
                (bins_hbm, bins_ref),
                (inner_hbm, inner),
                (pool_hbm, pool_ref),
            ]
        )
    ]
    for table in tables_in:
        table.start()
    load.wait()
    packed[:, :full] = raw[0, :full].T
    packed[:, full : 2 * full] = raw[1, :full].T
    if tail:
        packed[:, 2 * full :] = jnp.concatenate([raw[0, full:], raw[1, full:]], axis=0).T
    pl.semaphore_wait(barrier, outer + 1)

    def rows_of(line, i):
        return pl.ds(pl.multiple_of(line * columns + begins[i], 8), sizes[i])

    def part(i):
        return pl.ds(begins[i], sizes[i])

    incoming = {}
    for i in range(chunks):
        for step in range(outer - 1, 0, -1):
            there = lax.rem(me + step, outer)
            incoming[i, step] = pltpu.make_async_remote_copy(
                src_ref=packed.at[rows_of(there, i)],
                dst_ref=gathered.at[me, part(i)],
                send_sem=in_send.at[i, step],
                recv_sem=in_recv.at[i, step],
                device_id={"line": there},
                device_id_type=MESH,
            )
            incoming[i, step].start()
    gathered[me] = packed[pl.ds(pl.multiple_of(me * columns, 8), columns), :]

    for table in tables_in:
        table.wait()
    lower = start_ref[date]
    upper = stop_ref[date]
    bins = bins_ref[...]
    keep = (bins >= lower) & (bins < upper)
    lane = lax.broadcasted_iota(jnp.int32, bins.shape, 2)
    imaginary = ((lane >= full) & (lane < 2 * full)) | (lane >= 2 * full + tail)
    keep_conj = jnp.where(keep, jnp.where(imaginary, -1.0, 1.0), 0.0).astype(jnp.float32)

    def inner_dft(values):
        high, low = split(values)
        dot = functools.partial(jnp.dot, preferred_element_type=jnp.float32)
        return dot(high, inner[0]) + (dot(low, inner[0]) + dot(high, inner[1]))

    samples = width // LOOKS
    lines_all = outer * width
    out_lane = lax.broadcasted_iota(jnp.int32, (1, 2 * samples), 1)
    scale = 1.0 / (lines_all * lines_all * LOOKS)
    out_scale = jnp.where(out_lane < samples, scale, -scale).astype(jnp.float32)

    handed, outgoing = {}, {}

    def forward(i):
        for step in range(1, outer):
            incoming[i, step].wait_recv()
        rows = short_dft([as_row(gathered[l, part(i), :], full, tail) for l in range(outer)])
        rows = [rows[0]] + [twisted(rows[k], twist_ref[k], full, tail) for k in range(1, outer)]
        result = inner_dft(jnp.concatenate([row.flat() for row in rows], axis=0))
        spectrum[:, part(i), :] = result.reshape(outer, sizes[i], 2 * width)
        handed[i] = pltpu.make_async_remote_copy(
            src_ref=spectrum.at[:, part(i)],
            dst_ref=partner.at[:, part(i)],
            send_sem=date_send.at[i],
            recv_sem=date_recv.at[i],
            device_id={"date": previous},
            device_id_type=MESH,
        )
        handed[i].start()

    def signal(values, chunk):
        rows = []
        for k in range(outer):
            row = as_row(values[k * chunk : (k + 1) * chunk], full, tail)
            rows.append(twisted(row, twist_ref[k], full, tail) if k else row)
        return short_dft(rows)

    def backward(i):
        handed[i].wait_recv()
        chunk = sizes[i]
        both = jnp.concatenate(
            [spectrum[:, part(i), :] * keep_conj, partner[:, part(i), :] * keep_conj], axis=0
        )
        both = inner_dft(both.reshape(2 * outer * chunk, 2 * width))
        ref = signal(both[: outer * chunk], chunk)
        sec = signal(both[outer * chunk :], chunk)
        product = jnp.concatenate([times_conj(r, s).flat() for r, s in zip(ref, sec)], axis=0)
        high, low = split(product)
        weights = pool_ref[...]
        means = jnp.dot(high, weights, preferred_element_type=jnp.float32)
        means = (means + jnp.dot(low, weights, preferred_element_type=jnp.float32)) * out_scale
        looked[:, part(i), :] = means.reshape(outer, chunk, 2 * samples)
        for step in range(1, outer):
            there = lax.rem(me + step, outer)
            outgoing[i, step] = pltpu.make_async_remote_copy(
                src_ref=looked.at[there, part(i)],
                dst_ref=landed.at[rows_of(me, i)],
                send_sem=out_send.at[i, step],
                recv_sem=out_recv.at[i, step],
                device_id={"line": there},
                device_id_type=MESH,
            )
            outgoing[i, step].start()
        landed[rows_of(me, i), :] = looked[me, part(i), :]

    for i in range(chunks + 1):
        if i < chunks:
            forward(i)
        if i >= 1:
            backward(i - 1)

    for copy in outgoing.values():
        copy.wait_recv()
    out_ref[0] = landed[...].T.reshape(2, samples, columns_all)
    for copies in (incoming, handed, outgoing):
        for copy in copies.values():
            copy.wait_send()


def shards(slc, band_start, band_stop):
    outer = lax.axis_size("line")
    _, _, columns_all, width = slc.shape
    columns = columns_all // outer
    chunks = len(chunk_sizes(columns))
    samples = width // LOOKS
    inner, twist, bins, pool = (jnp.asarray(t) for t in tables(outer, width))
    vmem = pl.BlockSpec(memory_space=pltpu.VMEM)
    hbm = pl.BlockSpec(memory_space=pltpu.HBM)
    f32 = jnp.float32
    dma = pltpu.SemaphoreType.DMA
    result = pl.pallas_call(
        kernel,
        out_shape=pltpu.VMEM((1, 2, samples, columns_all), f32),
        in_specs=[hbm, hbm, hbm, hbm, hbm, hbm, hbm],
        out_specs=vmem,
        scratch_shapes=[
            pltpu.VMEM((2, width, columns_all), f32),
            pltpu.VMEM((columns_all, 2 * width), f32),
            pltpu.VMEM(inner.shape, jnp.bfloat16),
            pltpu.VMEM(twist.shape, f32),
            pltpu.VMEM(bins.shape, jnp.int32),
            pltpu.VMEM(pool.shape, jnp.bfloat16),
            pltpu.SMEM(band_start.shape, jnp.int32),
            pltpu.SMEM(band_stop.shape, jnp.int32),
            pltpu.VMEM((outer, columns, 2 * width), f32),
            pltpu.VMEM((outer, columns, 2 * width), f32),
            pltpu.VMEM((outer, columns, 2 * width), f32),
            pltpu.VMEM((outer, columns, 2 * samples), f32),
            pltpu.VMEM((columns_all, 2 * samples), f32),
            dma,
            dma((6,)),
            dma((chunks, outer)),
            dma((chunks, outer)),
            dma((chunks,)),
            dma((chunks,)),
            dma((chunks, outer)),
            dma((chunks, outer)),
        ],
        compiler_params=pltpu.CompilerParams(
            collective_id=0, has_side_effects=True, vmem_limit_bytes=66000000
        ),
    )(jnp.swapaxes(slc, 2, 3), inner, twist, bins, pool, band_start, band_stop)
    return jnp.swapaxes(result, 2, 3)


def solution(mesh):
    return jax.shard_map(
        shards,
        mesh=mesh,
        in_specs=(P("date", None, "stack", "line"), P(), P()),
        out_specs=P("date", None, "stack", "line"),
        check_vma=False,
    )
```

```python
import functools

import jax
import jax.numpy as jnp
import numpy as np
from jax import lax
from jax.experimental import pallas as pl
from jax.experimental.pallas import tpu as pltpu
from jax.sharding import PartitionSpec as P

LOOKS = 5
LANES = 128
MESH = pl.DeviceIdType.MESH
CHUNK = 16
SMALL = 16


def layout(width):
    full = width // LANES * LANES
    tail = width - full
    assert 2 * tail in (0, LANES)
    comp = np.concatenate([np.zeros(full), np.ones(full), np.zeros(tail), np.ones(tail)])
    index = np.concatenate([np.arange(full), np.arange(full), np.arange(tail) + full, np.arange(tail) + full])
    return full, tail, comp.astype(np.int64), index.astype(np.int64)


def split(values):
    high = values.astype(jnp.bfloat16)
    return high, (values - high.astype(jnp.float32)).astype(jnp.bfloat16)


def tables(outer, width):
    full, tail, comp, index = layout(width)
    angle = 2.0 * np.pi / width * (index[:, None] * index[None, :] % width)
    c, s = np.cos(angle), np.sin(angle)
    same = comp[:, None] == comp[None, :]
    to_re = (comp[:, None] == 1) & (comp[None, :] == 0)
    dense = np.where(same, c, np.where(to_re, s, -s)).astype(np.float32)
    high = dense.astype(jnp.bfloat16)
    low = (dense - high.astype(np.float32)).astype(jnp.bfloat16)
    inner = np.stack([high, low])
    lines = outer * width
    turn = 2.0 * np.pi / lines * (np.arange(outer)[:, None] * index[None, :] % lines)
    along = np.cos(turn)
    across = np.where(comp[None, :] == 0, np.sin(turn), -np.sin(turn))
    twist = np.stack([along, across], axis=1).astype(np.float32)
    bins = (np.arange(outer)[:, None] + outer * index[None, :]).astype(np.int32)[:, None, :]
    samples = width // LOOKS
    target = index // LOOKS + samples * comp
    pool = (target[:, None] == np.arange(2 * samples)[None, :]).astype(jnp.bfloat16)
    return inner, twist, bins, pool


def chunk_sizes(columns):
    sizes, left = [], columns
    while left > CHUNK and left % SMALL == 0:
        sizes.append(CHUNK)
        left -= CHUNK
    if left % SMALL == 0:
        return sizes + [SMALL] * (left // SMALL)
    return sizes + [left]


class Row:
    def __init__(self, re, im, tail):
        self.re, self.im, self.tail = re, im, tail

    def __add__(self, other):
        return Row(self.re + other.re, self.im + other.im, None if self.tail is None else self.tail + other.tail)

    def __sub__(self, other):
        return Row(self.re - other.re, self.im - other.im, None if self.tail is None else self.tail - other.tail)

    def flat(self):
        parts = [self.re, self.im] + ([] if self.tail is None else [self.tail])
        return jnp.concatenate(parts, axis=-1)


def as_row(values, full, tail):
    return Row(
        values[:, :full],
        values[:, full : 2 * full],
        values[:, 2 * full :] if tail else None,
    )


def swapped(tail_values):
    return pltpu.roll(tail_values, LANES // 2, 1)


def first_half(tail_values):
    return lax.broadcasted_iota(jnp.int32, tail_values.shape, 1) < LANES // 2


def times_minus_i(row):
    tail = row.tail
    if tail is not None:
        turned = swapped(tail)
        tail = jnp.where(first_half(tail), turned, -turned)
    return Row(row.im, -row.re, tail)


def times_phase(row, c, s):
    tail = row.tail
    if tail is not None:
        turned = swapped(tail) * s
        tail = tail * c + jnp.where(first_half(tail), turned, -turned)
    return Row(row.re * c + row.im * s, row.im * c - row.re * s, tail)


def short_dft(rows):
    count = len(rows)
    if count == 1:
        return rows
    if count % 2:
        result = []
        for k in range(count):
            total = rows[0]
            for n in range(1, count):
                angle = 2.0 * np.pi * (n * k % count) / count
                total = total + times_phase(rows[n], float(np.cos(angle)), float(np.sin(angle)))
            result.append(total)
        return result
    even, odd = short_dft(rows[0::2]), short_dft(rows[1::2])
    half = count // 2
    low, high = [], []
    for k in range(half):
        if k == 0:
            turned = odd[k]
        elif 4 * k == count:
            turned = times_minus_i(odd[k])
        else:
            angle = 2.0 * np.pi * k / count
            turned = times_phase(odd[k], float(np.cos(angle)), float(np.sin(angle)))
        low.append(even[k] + turned)
        high.append(even[k] - turned)
    return low + high


def twisted(row, twist, full, tail):
    along, across = twist[0:1, :], twist[1:2, :]
    tail_values = row.tail
    if tail_values is not None:
        tail_values = tail_values * along[:, 2 * full :] + swapped(tail_values) * across[:, 2 * full :]
    return Row(
        row.re * along[:, :full] + row.im * across[:, :full],
        row.im * along[:, :full] + row.re * across[:, full : 2 * full],
        tail_values,
    )


def times_conj(ref, sec):
    tail = None
    if ref.tail is not None:
        straight = ref.tail * sec.tail
        crossed = ref.tail * swapped(sec.tail)
        tail = jnp.where(
            first_half(straight), straight + swapped(straight), crossed - swapped(crossed)
        )
    return Row(
        ref.re * sec.re + ref.im * sec.im,
        ref.im * sec.re - ref.re * sec.im,
        tail,
    )


def kernel(
    slc_ref, inner_hbm, twist_hbm, bins_hbm, pool_hbm, start_hbm, stop_hbm, out_ref,
    raw, packed, inner, twist_ref, bins_ref, pool_ref, start_ref, stop_ref, gathered, spectrum, partner, looked, landed,
    load_sem, table_sem, in_send, in_recv, date_send, date_recv, out_send, out_recv,
):
    outer = lax.axis_size("line")
    dates = lax.axis_size("date")
    me = lax.axis_index("line")
    date = lax.axis_index("date")
    width, columns_all = raw.shape[1], raw.shape[2]
    columns = columns_all // outer
    sizes = chunk_sizes(columns)
    chunks = len(sizes)
    begins = [sum(sizes[:i]) for i in range(chunks)]
    full, tail, _, _ = layout(width)
    previous = lax.rem(date + dates - 1, dates)
    following = lax.rem(date + 1, dates)

    barrier = pltpu.get_barrier_semaphore()
    for step in range(1, outer):
        pl.semaphore_signal(
            barrier, inc=1, device_id={"line": lax.rem(me + step, outer)}, device_id_type=MESH
        )
    for other in (previous, following):
        pl.semaphore_signal(barrier, inc=1, device_id={"date": other}, device_id_type=MESH)

    load = pltpu.make_async_copy(slc_ref.at[0], raw, load_sem)
    load.start()
    tables_in = [
        pltpu.make_async_copy(source, target, table_sem.at[t])
        for t, (source, target) in enumerate(
            [
                (start_hbm, start_ref),
                (stop_hbm, stop_ref),
                (twist_hbm, twist_ref),
                (bins_hbm, bins_ref),
                (inner_hbm, inner),
                (pool_hbm, pool_ref),
            ]
        )
    ]
    for table in tables_in:
        table.start()
    load.wait()
    packed[:, :full] = raw[0, :full].T
    packed[:, full : 2 * full] = raw[1, :full].T
    if tail:
        packed[:, 2 * full :] = jnp.concatenate([raw[0, full:], raw[1, full:]], axis=0).T
    pl.semaphore_wait(barrier, outer + 1)

    def rows_of(line, i):
        return pl.ds(pl.multiple_of(line * columns + begins[i], 8), sizes[i])

    def part(i):
        return pl.ds(begins[i], sizes[i])

    incoming = {}
    for i in range(chunks):
        for step in range(outer - 1, 0, -1):
            there = lax.rem(me + step, outer)
            incoming[i, step] = pltpu.make_async_remote_copy(
                src_ref=packed.at[rows_of(there, i)],
                dst_ref=gathered.at[me, part(i)],
                send_sem=in_send.at[i, step],
                recv_sem=in_recv.at[i, step],
                device_id={"line": there},
                device_id_type=MESH,
            )
            incoming[i, step].start()
    gathered[me] = packed[pl.ds(pl.multiple_of(me * columns, 8), columns), :]

    for table in tables_in:
        table.wait()
    lower = start_ref[date]
    upper = stop_ref[date]
    bins = bins_ref[...]
    keep = (bins >= lower) & (bins < upper)
    lane = lax.broadcasted_iota(jnp.int32, bins.shape, 2)
    imaginary = ((lane >= full) & (lane < 2 * full)) | (lane >= 2 * full + tail)
    keep_conj = jnp.where(keep, jnp.where(imaginary, -1.0, 1.0), 0.0).astype(jnp.float32)

    def inner_dft(values):
        high, low = split(values)
        dot = functools.partial(jnp.dot, preferred_element_type=jnp.float32)
        return dot(high, inner[0]) + (dot(low, inner[0]) + dot(high, inner[1]))

    samples = width // LOOKS
    lines_all = outer * width
    out_lane = lax.broadcasted_iota(jnp.int32, (1, 2 * samples), 1)
    scale = 1.0 / (lines_all * lines_all * LOOKS)
    out_scale = jnp.where(out_lane < samples, scale, -scale).astype(jnp.float32)

    handed, outgoing = {}, {}

    def forward(i):
        for step in range(1, outer):
            incoming[i, step].wait_recv()
        rows = short_dft([as_row(gathered[l, part(i), :], full, tail) for l in range(outer)])
        rows = [rows[0]] + [twisted(rows[k], twist_ref[k], full, tail) for k in range(1, outer)]
        result = inner_dft(jnp.concatenate([row.flat() for row in rows], axis=0))
        spectrum[:, part(i), :] = result.reshape(outer, sizes[i], 2 * width)
        handed[i] = pltpu.make_async_remote_copy(
            src_ref=spectrum.at[:, part(i)],
            dst_ref=partner.at[:, part(i)],
            send_sem=date_send.at[i],
            recv_sem=date_recv.at[i],
            device_id={"date": previous},
            device_id_type=MESH,
        )
        handed[i].start()

    def signal(values, chunk):
        rows = []
        for k in range(outer):
            row = as_row(values[k * chunk : (k + 1) * chunk], full, tail)
            rows.append(twisted(row, twist_ref[k], full, tail) if k else row)
        return short_dft(rows)

    def backward(i):
        handed[i].wait_recv()
        chunk = sizes[i]
        both = jnp.concatenate(
            [spectrum[:, part(i), :] * keep_conj, partner[:, part(i), :] * keep_conj], axis=0
        )
        both = inner_dft(both.reshape(2 * outer * chunk, 2 * width))
        ref = signal(both[: outer * chunk], chunk)
        sec = signal(both[outer * chunk :], chunk)
        product = jnp.concatenate([times_conj(r, s).flat() for r, s in zip(ref, sec)], axis=0)
        high, low = split(product)
        weights = pool_ref[...]
        means = jnp.dot(high, weights, preferred_element_type=jnp.float32)
        means = (means + jnp.dot(low, weights, preferred_element_type=jnp.float32)) * out_scale
        looked[:, part(i), :] = means.reshape(outer, chunk, 2 * samples)
        for step in range(1, outer):
            there = lax.rem(me + step, outer)
            outgoing[i, step] = pltpu.make_async_remote_copy(
                src_ref=looked.at[there, part(i)],
                dst_ref=landed.at[rows_of(me, i)],
                send_sem=out_send.at[i, step],
                recv_sem=out_recv.at[i, step],
                device_id={"line": there},
                device_id_type=MESH,
            )
            outgoing[i, step].start()
        landed[rows_of(me, i), :] = looked[me, part(i), :]

    for i in range(chunks + 1):
        if i < chunks:
            forward(i)
        if i >= 1:
            backward(i - 1)

    for copy in outgoing.values():
        copy.wait_recv()
    out_ref[0] = landed[...].T.reshape(2, samples, columns_all)
    for copies in (incoming, handed, outgoing):
        for copy in copies.values():
            copy.wait_send()


def shards(slc, band_start, band_stop):
    outer = lax.axis_size("line")
    _, _, columns_all, width = slc.shape
    columns = columns_all // outer
    chunks = len(chunk_sizes(columns))
    samples = width // LOOKS
    inner, twist, bins, pool = (jnp.asarray(t) for t in tables(outer, width))
    vmem = pl.BlockSpec(memory_space=pltpu.VMEM)
    hbm = pl.BlockSpec(memory_space=pltpu.HBM)
    f32 = jnp.float32
    dma = pltpu.SemaphoreType.DMA
    result = pl.pallas_call(
        kernel,
        out_shape=pltpu.VMEM((1, 2, samples, columns_all), f32),
        in_specs=[hbm, hbm, hbm, hbm, hbm, hbm, hbm],
        out_specs=vmem,
        scratch_shapes=[
            pltpu.VMEM((2, width, columns_all), f32),
            pltpu.VMEM((columns_all, 2 * width), f32),
            pltpu.VMEM(inner.shape, jnp.bfloat16),
            pltpu.VMEM(twist.shape, f32),
            pltpu.VMEM(bins.shape, jnp.int32),
            pltpu.VMEM(pool.shape, jnp.bfloat16),
            pltpu.SMEM(band_start.shape, jnp.int32),
            pltpu.SMEM(band_stop.shape, jnp.int32),
            pltpu.VMEM((outer, columns, 2 * width), f32),
            pltpu.VMEM((outer, columns, 2 * width), f32),
            pltpu.VMEM((outer, columns, 2 * width), f32),
            pltpu.VMEM((outer, columns, 2 * samples), f32),
            pltpu.VMEM((columns_all, 2 * samples), f32),
            dma,
            dma((6,)),
            dma((chunks, outer)),
            dma((chunks, outer)),
            dma((chunks,)),
            dma((chunks,)),
            dma((chunks, outer)),
            dma((chunks, outer)),
        ],
        compiler_params=pltpu.CompilerParams(
            collective_id=0, has_side_effects=True, vmem_limit_bytes=66000000
        ),
    )(jnp.swapaxes(slc, 2, 3), inner, twist, bins, pool, band_start, band_stop)
    return jnp.swapaxes(result, 2, 3)


def shared_kernel(
    slc_ref, inner_hbm, twist_hbm, bins_hbm, pool_hbm, start_hbm, stop_hbm, out_ref,
    raw, packed, inner, twist_ref, bins_ref, pool_ref, start_ref, stop_ref, gathered, ref_signal, sec_signal, looked, landed,
    load_sem, table_sem, in_send, in_recv, out_send, out_recv,
):
    outer = lax.axis_size("line")
    dates = lax.axis_size("date")
    me = lax.axis_index("line")
    date = lax.axis_index("date")
    width, columns_all = raw.shape[1], raw.shape[2]
    columns = columns_all // (outer * dates)
    full, tail, _, _ = layout(width)
    slots = slot_dates(dates)
    steps = line_steps(outer)

    def at_date(relative):
        return lax.rem(date + relative, dates)

    def at_line(step):
        return lax.rem(me + step, outer)

    def device(relative, step):
        return {"date": at_date(relative), "line": at_line(step)}

    barrier = pltpu.get_barrier_semaphore()
    for relative in range(dates):
        for step in range(outer):
            if relative or step:
                pl.semaphore_signal(
                    barrier, inc=1, device_id=device(relative, step), device_id_type=MESH
                )

    load = pltpu.make_async_copy(slc_ref.at[0], raw, load_sem)
    load.start()
    tables_in = [
        pltpu.make_async_copy(source, target, table_sem.at[t])
        for t, (source, target) in enumerate(
            [
                (start_hbm, start_ref),
                (stop_hbm, stop_ref),
                (twist_hbm, twist_ref),
                (bins_hbm, bins_ref),
                (inner_hbm, inner),
                (pool_hbm, pool_ref),
            ]
        )
    ]
    for table in tables_in:
        table.start()
    load.wait()
    packed[:, :full] = raw[0, :full].T
    packed[:, full : 2 * full] = raw[1, :full].T
    if tail:
        packed[:, 2 * full :] = jnp.concatenate([raw[0, full:], raw[1, full:]], axis=0).T
    pl.semaphore_wait(barrier, outer * dates - 1)

    def rows_of(at, line, begin, size):
        return pl.ds(pl.multiple_of((at * outer + line) * columns + begin, 8), size)

    last = len(slots) - 1

    def parts(k):
        return last_parts(columns) if k == last else [(0, columns)]

    incoming = {}
    for k, relative in enumerate(slots):
        to = dates - relative if relative else 0
        for c, (begin, size) in enumerate(parts(k)):
            for step in steps:
                if to == 0 and step == 0:
                    continue
                incoming[k, c, step] = pltpu.make_async_remote_copy(
                    src_ref=packed.at[rows_of(at_date(to), at_line(step), begin, size)],
                    dst_ref=gathered.at[k, me, pl.ds(begin, size)],
                    send_sem=in_send.at[k, c, step],
                    recv_sem=in_recv.at[k, c, step],
                    device_id=device(to, step),
                    device_id_type=MESH,
                )
                incoming[k, c, step].start()
    gathered[slots.index(0), me] = packed[rows_of(date, me, 0, columns), :]

    for table in tables_in:
        table.wait()
    bins = bins_ref[...]
    lane = lax.broadcasted_iota(jnp.int32, bins.shape, 2)
    imaginary = ((lane >= full) & (lane < 2 * full)) | (lane >= 2 * full + tail)
    sign = jnp.where(imaginary, -1.0, 1.0).astype(jnp.float32)

    def keep_conj(relative):
        pair = at_date(relative)
        return jnp.where((bins >= start_ref[pair]) & (bins < stop_ref[pair]), sign, 0.0)

    def inner_dft(values):
        high, low = split(values)
        count = values.shape[0]
        both = jnp.dot(jnp.concatenate([high, low], axis=0), inner[0], preferred_element_type=jnp.float32)
        return both[:count] + (both[count:] + jnp.dot(high, inner[1], preferred_element_type=jnp.float32))

    samples = width // LOOKS
    lines_all = outer * width
    out_lane = lax.broadcasted_iota(jnp.int32, (1, 2 * samples), 1)
    scale = 1.0 / (lines_all * lines_all * LOOKS)
    out_scale = jnp.where(out_lane < samples, scale, -scale).astype(jnp.float32)

    def filtered(k, c):
        relative = slots[k]
        before = (relative + dates - 1) % dates
        begin, size = parts(k)[c]
        rows = pl.ds(begin, size)
        lines = short_dft([as_row(gathered[k, l, rows, :], full, tail) for l in range(outer)])
        lines = [lines[0]] + [twisted(lines[n], twist_ref[n], full, tail) for n in range(1, outer)]
        spectrum = inner_dft(jnp.concatenate([line.flat() for line in lines], axis=0))
        spectrum = spectrum.reshape(outer, size, 2 * width)
        both = jnp.concatenate([spectrum * keep_conj(relative), spectrum * keep_conj(before)], axis=0)
        both = inner_dft(both.reshape(2 * outer * size, 2 * width)).reshape(2 * outer, size, 2 * width)
        for base, target, pair in ((0, ref_signal, relative), (outer, sec_signal, before)):
            lines = []
            for n in range(outer):
                line = as_row(both[base + n], full, tail)
                lines.append(twisted(line, twist_ref[n], full, tail) if n else line)
            for n, line in enumerate(short_dft(lines)):
                target[pair, n, rows, :] = line.flat()

    def multilook(pair, begin, size):
        rows = pl.ds(begin, size)
        product = [
            times_conj(
                as_row(ref_signal[pair, n, rows, :], full, tail),
                as_row(sec_signal[pair, n, rows, :], full, tail),
            ).flat()
            for n in range(outer)
        ]
        high, low = split(jnp.concatenate(product, axis=0))
        means = jnp.dot(jnp.concatenate([high, low], axis=0), pool_ref[...], preferred_element_type=jnp.float32)
        means = (means[: outer * size] + means[outer * size :]) * out_scale
        looked[pair, :, rows, :] = means.reshape(outer, size, 2 * samples)

    outgoing = {}

    def send_out(pair, c, begin, size):
        for step in steps:
            if pair == 0 and step == 0:
                landed[rows_of(date, me, begin, size), :] = looked[0, me, pl.ds(begin, size), :]
                continue
            outgoing[pair, c, step] = pltpu.make_async_remote_copy(
                src_ref=looked.at[pair, at_line(step), pl.ds(begin, size)],
                dst_ref=landed.at[rows_of(date, me, begin, size)],
                send_sem=out_send.at[pair, c, step],
                recv_sem=out_recv.at[pair, c, step],
                device_id=device(pair, step),
                device_id_type=MESH,
            )
            outgoing[pair, c, step].start()

    def ready(k):
        have = slots[: k + 1]
        return [
            p for p in (slots[k], (slots[k] + dates - 1) % dates)
            if p in have and (p + 1) % dates in have
        ]

    held = []
    for k in range(len(slots)):
        for c, (begin, size) in enumerate(parts(k)):
            for step in steps:
                if (k, c, step) in incoming:
                    incoming[k, c, step].wait_recv()
            if k == last and c == len(parts(k)) - 1:
                for args in held:
                    send_out(*args)
                held = []
            filtered(k, c)
            done = sorted(set(ready(k)), key=lambda p: p == 0)
            for pair in done:
                multilook(pair, begin, size)
                held.append((pair, c, begin, size))
                if k == last and c == len(parts(k)) - 1:
                    send_out(*held.pop())

    for copy in outgoing.values():
        copy.wait_recv()
    out_ref[0] = landed[...].T.reshape(2, samples, columns_all)
    for copies in (incoming, outgoing):
        for copy in copies.values():
            copy.wait_send()


def slot_dates(dates):
    return list(range(1, dates, 2)) + list(range(2, dates, 2)) + [0]


def line_steps(outer):
    return sorted(range(outer), key=lambda step: (abs(2 * step - outer), step))


def last_parts(columns):
    half = columns // 2
    return [(0, columns)] if columns % 16 else [(0, half), (half, half)]


def shared_shards(slc, band_start, band_stop):
    outer = lax.axis_size("line")
    dates = lax.axis_size("date")
    _, _, columns_all, width = slc.shape
    columns = columns_all // (outer * dates)
    samples = width // LOOKS
    inner, twist, bins, pool = (jnp.asarray(t) for t in tables(outer, width))
    vmem = pl.BlockSpec(memory_space=pltpu.VMEM)
    hbm = pl.BlockSpec(memory_space=pltpu.HBM)
    f32 = jnp.float32
    dma = pltpu.SemaphoreType.DMA
    most = len(last_parts(columns))
    result = pl.pallas_call(
        shared_kernel,
        out_shape=pltpu.VMEM((1, 2, samples, columns_all), f32),
        in_specs=[hbm, hbm, hbm, hbm, hbm, hbm, hbm],
        out_specs=vmem,
        scratch_shapes=[
            pltpu.VMEM((2, width, columns_all), f32),
            pltpu.VMEM((columns_all, 2 * width), f32),
            pltpu.VMEM(inner.shape, jnp.bfloat16),
            pltpu.VMEM(twist.shape, f32),
            pltpu.VMEM(bins.shape, jnp.int32),
            pltpu.VMEM(pool.shape, jnp.bfloat16),
            pltpu.SMEM(band_start.shape, jnp.int32),
            pltpu.SMEM(band_stop.shape, jnp.int32),
            pltpu.VMEM((dates, outer, columns, 2 * width), f32),
            pltpu.VMEM((dates, outer, columns, 2 * width), f32),
            pltpu.VMEM((dates, outer, columns, 2 * width), f32),
            pltpu.VMEM((dates, outer, columns, 2 * samples), f32),
            pltpu.VMEM((columns_all, 2 * samples), f32),
            dma,
            dma((6,)),
            dma((dates, most, outer)),
            dma((dates, most, outer)),
            dma((dates, most, outer)),
            dma((dates, most, outer)),
        ],
        compiler_params=pltpu.CompilerParams(
            collective_id=0, has_side_effects=True, vmem_limit_bytes=66000000
        ),
    )(jnp.swapaxes(slc, 2, 3), inner, twist, bins, pool, band_start, band_stop)
    return jnp.swapaxes(result, 2, 3)


def solution(mesh):
    group = mesh.shape["line"] * mesh.shape["date"]

    def body(slc, band_start, band_stop):
        shared = mesh.shape["date"] > 1 and slc.shape[2] % (8 * group) == 0
        return (shared_shards if shared else shards)(slc, band_start, band_stop)

    return jax.shard_map(
        body,
        mesh=mesh,
        in_specs=(P("date", None, "stack", "line"), P(), P()),
        out_specs=P("date", None, "stack", "line"),
        check_vma=False,
    )
```

```python
import functools

import jax
import jax.numpy as jnp
import numpy as np
from jax import lax
from jax.experimental import pallas as pl
from jax.experimental.pallas import tpu as pltpu
from jax.sharding import PartitionSpec as P

LOOKS = 5
LANES = 128
MESH = pl.DeviceIdType.MESH
CHUNK = 16
SMALL = 16


def layout(width):
    full = width // LANES * LANES
    tail = width - full
    assert 2 * tail in (0, LANES)
    comp = np.concatenate([np.zeros(full), np.ones(full), np.zeros(tail), np.ones(tail)])
    index = np.concatenate([np.arange(full), np.arange(full), np.arange(tail) + full, np.arange(tail) + full])
    return full, tail, comp.astype(np.int64), index.astype(np.int64)


def split(values):
    high = values.astype(jnp.bfloat16)
    return high, (values - high.astype(jnp.float32)).astype(jnp.bfloat16)


def tables(outer, width):
    full, tail, comp, index = layout(width)
    angle = 2.0 * np.pi / width * (index[:, None] * index[None, :] % width)
    c, s = np.cos(angle), np.sin(angle)
    same = comp[:, None] == comp[None, :]
    to_re = (comp[:, None] == 1) & (comp[None, :] == 0)
    dense = np.where(same, c, np.where(to_re, s, -s)).astype(np.float32)
    high = dense.astype(jnp.bfloat16)
    low = (dense - high.astype(np.float32)).astype(jnp.bfloat16)
    inner = np.stack([high, low])
    lines = outer * width
    turn = 2.0 * np.pi / lines * (np.arange(outer)[:, None] * index[None, :] % lines)
    along = np.cos(turn)
    across = np.where(comp[None, :] == 0, np.sin(turn), -np.sin(turn))
    twist = np.stack([along, across], axis=1).astype(np.float32)
    bins = (np.arange(outer)[:, None] + outer * index[None, :]).astype(np.int32)[:, None, :]
    samples = width // LOOKS
    target = index // LOOKS + samples * comp
    pool = (target[:, None] == np.arange(2 * samples)[None, :]).astype(jnp.bfloat16)
    return inner, twist, bins, pool


def chunk_sizes(columns):
    sizes, left = [], columns
    while left > CHUNK and left % SMALL == 0:
        sizes.append(CHUNK)
        left -= CHUNK
    if left % SMALL == 0:
        return sizes + [SMALL] * (left // SMALL)
    return sizes + [left]


class Row:
    def __init__(self, re, im, tail):
        self.re, self.im, self.tail = re, im, tail

    def __add__(self, other):
        return Row(self.re + other.re, self.im + other.im, None if self.tail is None else self.tail + other.tail)

    def __sub__(self, other):
        return Row(self.re - other.re, self.im - other.im, None if self.tail is None else self.tail - other.tail)

    def flat(self):
        parts = [self.re, self.im] + ([] if self.tail is None else [self.tail])
        return jnp.concatenate(parts, axis=-1)


def as_row(values, full, tail):
    return Row(
        values[:, :full],
        values[:, full : 2 * full],
        values[:, 2 * full :] if tail else None,
    )


def swapped(tail_values):
    return pltpu.roll(tail_values, LANES // 2, 1)


def first_half(tail_values):
    return lax.broadcasted_iota(jnp.int32, tail_values.shape, 1) < LANES // 2


def times_minus_i(row):
    tail = row.tail
    if tail is not None:
        turned = swapped(tail)
        tail = jnp.where(first_half(tail), turned, -turned)
    return Row(row.im, -row.re, tail)


def times_phase(row, c, s):
    tail = row.tail
    if tail is not None:
        turned = swapped(tail) * s
        tail = tail * c + jnp.where(first_half(tail), turned, -turned)
    return Row(row.re * c + row.im * s, row.im * c - row.re * s, tail)


def short_dft(rows):
    count = len(rows)
    if count == 1:
        return rows
    if count % 2:
        result = []
        for k in range(count):
            total = rows[0]
            for n in range(1, count):
                angle = 2.0 * np.pi * (n * k % count) / count
                total = total + times_phase(rows[n], float(np.cos(angle)), float(np.sin(angle)))
            result.append(total)
        return result
    even, odd = short_dft(rows[0::2]), short_dft(rows[1::2])
    half = count // 2
    low, high = [], []
    for k in range(half):
        if k == 0:
            turned = odd[k]
        elif 4 * k == count:
            turned = times_minus_i(odd[k])
        else:
            angle = 2.0 * np.pi * k / count
            turned = times_phase(odd[k], float(np.cos(angle)), float(np.sin(angle)))
        low.append(even[k] + turned)
        high.append(even[k] - turned)
    return low + high


def twisted(row, twist, full, tail):
    along, across = twist[0:1, :], twist[1:2, :]
    tail_values = row.tail
    if tail_values is not None:
        tail_values = tail_values * along[:, 2 * full :] + swapped(tail_values) * across[:, 2 * full :]
    return Row(
        row.re * along[:, :full] + row.im * across[:, :full],
        row.im * along[:, :full] + row.re * across[:, full : 2 * full],
        tail_values,
    )


def times_conj(ref, sec):
    tail = None
    if ref.tail is not None:
        straight = ref.tail * sec.tail
        crossed = ref.tail * swapped(sec.tail)
        tail = jnp.where(
            first_half(straight), straight + swapped(straight), crossed - swapped(crossed)
        )
    return Row(
        ref.re * sec.re + ref.im * sec.im,
        ref.im * sec.re - ref.re * sec.im,
        tail,
    )


def kernel(
    slc_ref, inner_hbm, twist_hbm, bins_hbm, pool_hbm, start_hbm, stop_hbm, out_ref,
    raw, packed, inner, twist_ref, bins_ref, pool_ref, start_ref, stop_ref, gathered, spectrum, partner, looked, landed,
    load_sem, table_sem, in_send, in_recv, date_send, date_recv, out_send, out_recv,
):
    outer = lax.axis_size("line")
    dates = lax.axis_size("date")
    me = lax.axis_index("line")
    date = lax.axis_index("date")
    width, columns_all = raw.shape[1], raw.shape[2]
    columns = columns_all // outer
    sizes = chunk_sizes(columns)
    chunks = len(sizes)
    begins = [sum(sizes[:i]) for i in range(chunks)]
    full, tail, _, _ = layout(width)
    previous = lax.rem(date + dates - 1, dates)
    following = lax.rem(date + 1, dates)

    barrier = pltpu.get_barrier_semaphore()
    for step in range(1, outer):
        pl.semaphore_signal(
            barrier, inc=1, device_id={"line": lax.rem(me + step, outer)}, device_id_type=MESH
        )
    for other in (previous, following):
        pl.semaphore_signal(barrier, inc=1, device_id={"date": other}, device_id_type=MESH)

    load = pltpu.make_async_copy(slc_ref.at[0], raw, load_sem)
    load.start()
    tables_in = [
        pltpu.make_async_copy(source, target, table_sem.at[t])
        for t, (source, target) in enumerate(
            [
                (start_hbm, start_ref),
                (stop_hbm, stop_ref),
                (twist_hbm, twist_ref),
                (bins_hbm, bins_ref),
                (inner_hbm, inner),
                (pool_hbm, pool_ref),
            ]
        )
    ]
    for table in tables_in:
        table.start()
    load.wait()
    packed[:, :full] = raw[0, :full].T
    packed[:, full : 2 * full] = raw[1, :full].T
    if tail:
        packed[:, 2 * full :] = jnp.concatenate([raw[0, full:], raw[1, full:]], axis=0).T
    pl.semaphore_wait(barrier, outer + 1)

    def rows_of(line, i):
        return pl.ds(pl.multiple_of(line * columns + begins[i], 8), sizes[i])

    def part(i):
        return pl.ds(begins[i], sizes[i])

    incoming = {}
    for i in range(chunks):
        for step in range(outer - 1, 0, -1):
            there = lax.rem(me + step, outer)
            incoming[i, step] = pltpu.make_async_remote_copy(
                src_ref=packed.at[rows_of(there, i)],
                dst_ref=gathered.at[me, part(i)],
                send_sem=in_send.at[i, step],
                recv_sem=in_recv.at[i, step],
                device_id={"line": there},
                device_id_type=MESH,
            )
            incoming[i, step].start()
    gathered[me] = packed[pl.ds(pl.multiple_of(me * columns, 8), columns), :]

    for table in tables_in:
        table.wait()
    lower = start_ref[date]
    upper = stop_ref[date]
    bins = bins_ref[...]
    keep = (bins >= lower) & (bins < upper)
    lane = lax.broadcasted_iota(jnp.int32, bins.shape, 2)
    imaginary = ((lane >= full) & (lane < 2 * full)) | (lane >= 2 * full + tail)
    keep_conj = jnp.where(keep, jnp.where(imaginary, -1.0, 1.0), 0.0).astype(jnp.float32)

    def inner_dft(values):
        high, low = split(values)
        dot = functools.partial(jnp.dot, preferred_element_type=jnp.float32)
        return dot(high, inner[0]) + (dot(low, inner[0]) + dot(high, inner[1]))

    samples = width // LOOKS
    lines_all = outer * width
    out_lane = lax.broadcasted_iota(jnp.int32, (1, 2 * samples), 1)
    scale = 1.0 / (lines_all * lines_all * LOOKS)
    out_scale = jnp.where(out_lane < samples, scale, -scale).astype(jnp.float32)

    handed, outgoing = {}, {}

    def forward(i):
        for step in range(1, outer):
            incoming[i, step].wait_recv()
        rows = short_dft([as_row(gathered[l, part(i), :], full, tail) for l in range(outer)])
        rows = [rows[0]] + [twisted(rows[k], twist_ref[k], full, tail) for k in range(1, outer)]
        result = inner_dft(jnp.concatenate([row.flat() for row in rows], axis=0))
        spectrum[:, part(i), :] = result.reshape(outer, sizes[i], 2 * width)
        handed[i] = pltpu.make_async_remote_copy(
            src_ref=spectrum.at[:, part(i)],
            dst_ref=partner.at[:, part(i)],
            send_sem=date_send.at[i],
            recv_sem=date_recv.at[i],
            device_id={"date": previous},
            device_id_type=MESH,
        )
        handed[i].start()

    def signal(values, chunk):
        rows = []
        for k in range(outer):
            row = as_row(values[k * chunk : (k + 1) * chunk], full, tail)
            rows.append(twisted(row, twist_ref[k], full, tail) if k else row)
        return short_dft(rows)

    def backward(i):
        handed[i].wait_recv()
        chunk = sizes[i]
        both = jnp.concatenate(
            [spectrum[:, part(i), :] * keep_conj, partner[:, part(i), :] * keep_conj], axis=0
        )
        both = inner_dft(both.reshape(2 * outer * chunk, 2 * width))
        ref = signal(both[: outer * chunk], chunk)
        sec = signal(both[outer * chunk :], chunk)
        product = jnp.concatenate([times_conj(r, s).flat() for r, s in zip(ref, sec)], axis=0)
        high, low = split(product)
        weights = pool_ref[...]
        means = jnp.dot(high, weights, preferred_element_type=jnp.float32)
        means = (means + jnp.dot(low, weights, preferred_element_type=jnp.float32)) * out_scale
        looked[:, part(i), :] = means.reshape(outer, chunk, 2 * samples)
        for step in range(1, outer):
            there = lax.rem(me + step, outer)
            outgoing[i, step] = pltpu.make_async_remote_copy(
                src_ref=looked.at[there, part(i)],
                dst_ref=landed.at[rows_of(me, i)],
                send_sem=out_send.at[i, step],
                recv_sem=out_recv.at[i, step],
                device_id={"line": there},
                device_id_type=MESH,
            )
            outgoing[i, step].start()
        landed[rows_of(me, i), :] = looked[me, part(i), :]

    for i in range(chunks + 1):
        if i < chunks:
            forward(i)
        if i >= 1:
            backward(i - 1)

    for copy in outgoing.values():
        copy.wait_recv()
    out_ref[0] = landed[...].T.reshape(2, samples, columns_all)
    for copies in (incoming, handed, outgoing):
        for copy in copies.values():
            copy.wait_send()


def shards(slc, band_start, band_stop):
    outer = lax.axis_size("line")
    _, _, columns_all, width = slc.shape
    columns = columns_all // outer
    chunks = len(chunk_sizes(columns))
    samples = width // LOOKS
    inner, twist, bins, pool = (jnp.asarray(t) for t in tables(outer, width))
    vmem = pl.BlockSpec(memory_space=pltpu.VMEM)
    hbm = pl.BlockSpec(memory_space=pltpu.HBM)
    f32 = jnp.float32
    dma = pltpu.SemaphoreType.DMA
    result = pl.pallas_call(
        kernel,
        out_shape=pltpu.VMEM((1, 2, samples, columns_all), f32),
        in_specs=[hbm, hbm, hbm, hbm, hbm, hbm, hbm],
        out_specs=vmem,
        scratch_shapes=[
            pltpu.VMEM((2, width, columns_all), f32),
            pltpu.VMEM((columns_all, 2 * width), f32),
            pltpu.VMEM(inner.shape, jnp.bfloat16),
            pltpu.VMEM(twist.shape, f32),
            pltpu.VMEM(bins.shape, jnp.int32),
            pltpu.VMEM(pool.shape, jnp.bfloat16),
            pltpu.SMEM(band_start.shape, jnp.int32),
            pltpu.SMEM(band_stop.shape, jnp.int32),
            pltpu.VMEM((outer, columns, 2 * width), f32),
            pltpu.VMEM((outer, columns, 2 * width), f32),
            pltpu.VMEM((outer, columns, 2 * width), f32),
            pltpu.VMEM((outer, columns, 2 * samples), f32),
            pltpu.VMEM((columns_all, 2 * samples), f32),
            dma,
            dma((6,)),
            dma((chunks, outer)),
            dma((chunks, outer)),
            dma((chunks,)),
            dma((chunks,)),
            dma((chunks, outer)),
            dma((chunks, outer)),
        ],
        compiler_params=pltpu.CompilerParams(
            collective_id=0, has_side_effects=True, vmem_limit_bytes=66000000
        ),
    )(jnp.swapaxes(slc, 2, 3), inner, twist, bins, pool, band_start, band_stop)
    return jnp.swapaxes(result, 2, 3)


def shared_kernel(
    slc_ref, inner_hbm, twist_hbm, bins_hbm, pool_hbm, start_hbm, stop_hbm, out_ref,
    raw, packed, inner, twist_ref, bins_ref, pool_ref, start_ref, stop_ref, gathered, ref_signal, sec_signal, looked, landed,
    load_sem, table_sem, in_send, in_recv, out_send, out_recv,
):
    outer = lax.axis_size("line")
    dates = lax.axis_size("date")
    me = lax.axis_index("line")
    date = lax.axis_index("date")
    width, columns_all = raw.shape[1], raw.shape[2]
    columns = columns_all // (outer * dates)
    full, tail, _, _ = layout(width)
    slots = slot_dates(dates)
    def at_date(relative):
        return lax.rem(date + relative, dates)

    def at_line(step):
        return lax.rem(me + step, outer)

    def device(relative, step):
        return {"date": at_date(relative), "line": at_line(step)}

    barrier = pltpu.get_barrier_semaphore()
    for relative in range(dates):
        for step in range(outer):
            if relative or step:
                pl.semaphore_signal(
                    barrier, inc=1, device_id=device(relative, step), device_id_type=MESH
                )

    load = pltpu.make_async_copy(slc_ref.at[0], raw, load_sem)
    load.start()
    tables_in = [
        pltpu.make_async_copy(source, target, table_sem.at[t])
        for t, (source, target) in enumerate(
            [
                (start_hbm, start_ref),
                (stop_hbm, stop_ref),
                (twist_hbm, twist_ref),
                (bins_hbm, bins_ref),
                (inner_hbm, inner),
                (pool_hbm, pool_ref),
            ]
        )
    ]
    for table in tables_in:
        table.start()
    load.wait()
    packed[:, :full] = raw[0, :full].T
    packed[:, full : 2 * full] = raw[1, :full].T
    if tail:
        packed[:, 2 * full :] = jnp.concatenate([raw[0, full:], raw[1, full:]], axis=0).T

    pl.semaphore_wait(barrier, outer * dates - 1)

    def rows_of(at, line):
        return pl.ds(pl.multiple_of((at * outer + line) * columns, 8), columns)

    incoming = {}
    for k, relative in enumerate(slots):
        to = (dates - relative) % dates
        for step in range(outer - 1, -1, -1):
            if to or step:
                incoming[k, step] = pltpu.make_async_remote_copy(
                    src_ref=packed.at[rows_of(at_date(to), at_line(step))],
                    dst_ref=gathered.at[k, me],
                    send_sem=in_send.at[k, step],
                    recv_sem=in_recv.at[k, step],
                    device_id=device(to, step),
                    device_id_type=MESH,
                )
                incoming[k, step].start()
    gathered[slots.index(0), me] = packed[rows_of(date, me), :]

    for table in tables_in:
        table.wait()
    bins = bins_ref[...]
    lane = lax.broadcasted_iota(jnp.int32, bins.shape, 2)
    imaginary = ((lane >= full) & (lane < 2 * full)) | (lane >= 2 * full + tail)
    sign = jnp.where(imaginary, -1.0, 1.0).astype(jnp.float32)

    def keep_conj(relative):
        pair = at_date(relative)
        return jnp.where((bins >= start_ref[pair]) & (bins < stop_ref[pair]), sign, 0.0)

    def inner_dft(values):
        high, low = split(values)
        count = values.shape[0]
        both = jnp.dot(jnp.concatenate([high, low], axis=0), inner[0], preferred_element_type=jnp.float32)
        return both[:count] + (both[count:] + jnp.dot(high, inner[1], preferred_element_type=jnp.float32))

    samples = width // LOOKS
    lines_all = outer * width
    out_lane = lax.broadcasted_iota(jnp.int32, (1, 2 * samples), 1)
    scale = 1.0 / (lines_all * lines_all * LOOKS)
    out_scale = jnp.where(out_lane < samples, scale, -scale).astype(jnp.float32)

    def filtered(k):
        relative = slots[k]
        before = (relative + dates - 1) % dates
        lines = short_dft([as_row(gathered[k, l], full, tail) for l in range(outer)])
        lines = [lines[0]] + [twisted(lines[n], twist_ref[n], full, tail) for n in range(1, outer)]
        spectrum = inner_dft(jnp.concatenate([line.flat() for line in lines], axis=0))
        spectrum = spectrum.reshape(outer, columns, 2 * width)
        both = jnp.concatenate([spectrum * keep_conj(relative), spectrum * keep_conj(before)], axis=0)
        both = inner_dft(both.reshape(2 * outer * columns, 2 * width))
        both = both.reshape(2 * outer, columns, 2 * width)
        for base, target, pair in ((0, ref_signal, relative), (outer, sec_signal, before)):
            lines = []
            for n in range(outer):
                line = as_row(both[base + n], full, tail)
                lines.append(twisted(line, twist_ref[n], full, tail) if n else line)
            for n, line in enumerate(short_dft(lines)):
                target[pair, n] = line.flat()

    def multilook(pair):
        product = [
            times_conj(
                as_row(ref_signal[pair, n], full, tail), as_row(sec_signal[pair, n], full, tail)
            ).flat()
            for n in range(outer)
        ]
        high, low = split(jnp.concatenate(product, axis=0))
        means = jnp.dot(jnp.concatenate([high, low], axis=0), pool_ref[...], preferred_element_type=jnp.float32)
        means = (means[: outer * columns] + means[outer * columns :]) * out_scale
        looked[pair] = means.reshape(outer, columns, 2 * samples)

    outgoing = {}

    def send_out(pair):
        for step in [*range(1, outer), 0]:
            if pair == 0 and step == 0:
                landed[rows_of(date, me), :] = looked[0, me]
                continue
            outgoing[pair, step] = pltpu.make_async_remote_copy(
                src_ref=looked.at[pair, at_line(step)],
                dst_ref=landed.at[rows_of(date, me)],
                send_sem=out_send.at[pair, step],
                recv_sem=out_recv.at[pair, step],
                device_id=device(pair, step),
                device_id_type=MESH,
            )
            outgoing[pair, step].start()

    def ready(k):
        have = slots[: k + 1]
        pairs = {slots[k], (slots[k] + dates - 1) % dates}
        return sorted((p for p in pairs if p in have and (p + 1) % dates in have), key=lambda p: p == 0)

    held = []
    for k in range(len(slots)):
        for step in range(outer):
            if (k, step) in incoming:
                incoming[k, step].wait_recv()
        final = k == len(slots) - 1
        if final:
            for pair in held:
                send_out(pair)
        filtered(k)
        for pair in ready(k):
            multilook(pair)
            if final:
                send_out(pair)
            else:
                held.append(pair)

    for copy in outgoing.values():
        copy.wait_recv()
    out_ref[0] = landed[...].T.reshape(2, samples, columns_all)
    for copies in (incoming, outgoing):
        for copy in copies.values():
            copy.wait_send()


def slot_dates(dates):
    return list(range(1, dates, 2)) + list(range(2, dates, 2)) + [0]


def shared_shards(slc, band_start, band_stop):
    outer = lax.axis_size("line")
    dates = lax.axis_size("date")
    _, _, columns_all, width = slc.shape
    columns = columns_all // (outer * dates)
    samples = width // LOOKS
    inner, twist, bins, pool = (jnp.asarray(t) for t in tables(outer, width))
    vmem = pl.BlockSpec(memory_space=pltpu.VMEM)
    hbm = pl.BlockSpec(memory_space=pltpu.HBM)
    f32 = jnp.float32
    dma = pltpu.SemaphoreType.DMA
    result = pl.pallas_call(
        shared_kernel,
        out_shape=pltpu.VMEM((1, 2, samples, columns_all), f32),
        in_specs=[hbm, hbm, hbm, hbm, hbm, hbm, hbm],
        out_specs=vmem,
        scratch_shapes=[
            pltpu.VMEM((2, width, columns_all), f32),
            pltpu.VMEM((columns_all, 2 * width), f32),
            pltpu.VMEM(inner.shape, jnp.bfloat16),
            pltpu.VMEM(twist.shape, f32),
            pltpu.VMEM(bins.shape, jnp.int32),
            pltpu.VMEM(pool.shape, jnp.bfloat16),
            pltpu.SMEM(band_start.shape, jnp.int32),
            pltpu.SMEM(band_stop.shape, jnp.int32),
            pltpu.VMEM((dates, outer, columns, 2 * width), f32),
            pltpu.VMEM((dates, outer, columns, 2 * width), f32),
            pltpu.VMEM((dates, outer, columns, 2 * width), f32),
            pltpu.VMEM((dates, outer, columns, 2 * samples), f32),
            pltpu.VMEM((columns_all, 2 * samples), f32),
            dma,
            dma((6,)),
            dma((dates, outer)),
            dma((dates, outer)),
            dma((dates, outer)),
            dma((dates, outer)),
        ],
        compiler_params=pltpu.CompilerParams(
            collective_id=0, has_side_effects=True, vmem_limit_bytes=66000000
        ),
    )(jnp.swapaxes(slc, 2, 3), inner, twist, bins, pool, band_start, band_stop)
    return jnp.swapaxes(result, 2, 3)


def solution(mesh):
    group = mesh.shape["line"] * mesh.shape["date"]

    def body(slc, band_start, band_stop):
        shared = slc.shape[2] % (8 * group) == 0
        return (shared_shards if shared else shards)(slc, band_start, band_stop)

    return jax.shard_map(
        body,
        mesh=mesh,
        in_specs=(P("date", None, "stack", "line"), P(), P()),
        out_specs=P("date", None, "stack", "line"),
        check_vma=False,
    )
```

```python
import functools

import jax
import jax.numpy as jnp
import numpy as np
from jax import lax
from jax.experimental import pallas as pl
from jax.experimental.pallas import tpu as pltpu
from jax.sharding import PartitionSpec as P

LOOKS = 5
LANES = 128
MESH = pl.DeviceIdType.MESH
CHUNK = 16
SMALL = 16


def layout(width):
    full = width // LANES * LANES
    tail = width - full
    assert 2 * tail in (0, LANES)
    comp = np.concatenate([np.zeros(full), np.ones(full), np.zeros(tail), np.ones(tail)])
    index = np.concatenate([np.arange(full), np.arange(full), np.arange(tail) + full, np.arange(tail) + full])
    return full, tail, comp.astype(np.int64), index.astype(np.int64)


def split(values):
    high = values.astype(jnp.bfloat16)
    return high, (values - high.astype(jnp.float32)).astype(jnp.bfloat16)


def tables(outer, width):
    full, tail, comp, index = layout(width)
    angle = 2.0 * np.pi / width * (index[:, None] * index[None, :] % width)
    c, s = np.cos(angle), np.sin(angle)
    same = comp[:, None] == comp[None, :]
    to_re = (comp[:, None] == 1) & (comp[None, :] == 0)
    dense = np.where(same, c, np.where(to_re, s, -s)).astype(np.float32)
    high = dense.astype(jnp.bfloat16)
    low = (dense - high.astype(np.float32)).astype(jnp.bfloat16)
    inner = np.stack([high, low])
    lines = outer * width
    turn = 2.0 * np.pi / lines * (np.arange(outer)[:, None] * index[None, :] % lines)
    along = np.cos(turn)
    across = np.where(comp[None, :] == 0, np.sin(turn), -np.sin(turn))
    twist = np.stack([along, across], axis=1).astype(np.float32)
    bins = (np.arange(outer)[:, None] + outer * index[None, :]).astype(np.int32)[:, None, :]
    samples = width // LOOKS
    target = index // LOOKS + samples * comp
    pool = (target[:, None] == np.arange(2 * samples)[None, :]).astype(jnp.bfloat16)
    return inner, twist, bins, pool


def chunk_sizes(columns):
    sizes, left = [], columns
    while left > CHUNK and left % SMALL == 0:
        sizes.append(CHUNK)
        left -= CHUNK
    if left % SMALL == 0:
        return sizes + [SMALL] * (left // SMALL)
    return sizes + [left]


class Row:
    def __init__(self, re, im, tail):
        self.re, self.im, self.tail = re, im, tail

    def __add__(self, other):
        return Row(self.re + other.re, self.im + other.im, None if self.tail is None else self.tail + other.tail)

    def __sub__(self, other):
        return Row(self.re - other.re, self.im - other.im, None if self.tail is None else self.tail - other.tail)

    def flat(self):
        parts = [self.re, self.im] + ([] if self.tail is None else [self.tail])
        return jnp.concatenate(parts, axis=-1)


def as_row(values, full, tail):
    return Row(
        values[:, :full],
        values[:, full : 2 * full],
        values[:, 2 * full :] if tail else None,
    )


def swapped(tail_values):
    return pltpu.roll(tail_values, LANES // 2, 1)


def first_half(tail_values):
    return lax.broadcasted_iota(jnp.int32, tail_values.shape, 1) < LANES // 2


def times_minus_i(row):
    tail = row.tail
    if tail is not None:
        turned = swapped(tail)
        tail = jnp.where(first_half(tail), turned, -turned)
    return Row(row.im, -row.re, tail)


def times_phase(row, c, s):
    tail = row.tail
    if tail is not None:
        turned = swapped(tail) * s
        tail = tail * c + jnp.where(first_half(tail), turned, -turned)
    return Row(row.re * c + row.im * s, row.im * c - row.re * s, tail)


def short_dft(rows):
    count = len(rows)
    if count == 1:
        return rows
    if count % 2:
        result = []
        for k in range(count):
            total = rows[0]
            for n in range(1, count):
                angle = 2.0 * np.pi * (n * k % count) / count
                total = total + times_phase(rows[n], float(np.cos(angle)), float(np.sin(angle)))
            result.append(total)
        return result
    even, odd = short_dft(rows[0::2]), short_dft(rows[1::2])
    half = count // 2
    low, high = [], []
    for k in range(half):
        if k == 0:
            turned = odd[k]
        elif 4 * k == count:
            turned = times_minus_i(odd[k])
        else:
            angle = 2.0 * np.pi * k / count
            turned = times_phase(odd[k], float(np.cos(angle)), float(np.sin(angle)))
        low.append(even[k] + turned)
        high.append(even[k] - turned)
    return low + high


def twisted(row, twist, full, tail):
    along, across = twist[0:1, :], twist[1:2, :]
    tail_values = row.tail
    if tail_values is not None:
        tail_values = tail_values * along[:, 2 * full :] + swapped(tail_values) * across[:, 2 * full :]
    return Row(
        row.re * along[:, :full] + row.im * across[:, :full],
        row.im * along[:, :full] + row.re * across[:, full : 2 * full],
        tail_values,
    )


def times_conj(ref, sec):
    tail = None
    if ref.tail is not None:
        straight = ref.tail * sec.tail
        crossed = ref.tail * swapped(sec.tail)
        tail = jnp.where(
            first_half(straight), straight + swapped(straight), crossed - swapped(crossed)
        )
    return Row(
        ref.re * sec.re + ref.im * sec.im,
        ref.im * sec.re - ref.re * sec.im,
        tail,
    )


def kernel(
    slc_ref, inner_hbm, twist_hbm, bins_hbm, pool_hbm, start_hbm, stop_hbm, out_ref,
    raw, packed, inner, twist_ref, bins_ref, pool_ref, start_ref, stop_ref, gathered, spectrum, partner, looked, landed,
    load_sem, table_sem, in_send, in_recv, date_send, date_recv, out_send, out_recv,
):
    outer = lax.axis_size("line")
    dates = lax.axis_size("date")
    me = lax.axis_index("line")
    date = lax.axis_index("date")
    width, columns_all = raw.shape[1], raw.shape[2]
    columns = columns_all // outer
    sizes = chunk_sizes(columns)
    chunks = len(sizes)
    begins = [sum(sizes[:i]) for i in range(chunks)]
    full, tail, _, _ = layout(width)
    previous = lax.rem(date + dates - 1, dates)
    following = lax.rem(date + 1, dates)

    barrier = pltpu.get_barrier_semaphore()
    for step in range(1, outer):
        pl.semaphore_signal(
            barrier, inc=1, device_id={"line": lax.rem(me + step, outer)}, device_id_type=MESH
        )
    for other in (previous, following):
        pl.semaphore_signal(barrier, inc=1, device_id={"date": other}, device_id_type=MESH)

    load = pltpu.make_async_copy(slc_ref.at[0], raw, load_sem)
    load.start()
    tables_in = [
        pltpu.make_async_copy(source, target, table_sem.at[t])
        for t, (source, target) in enumerate(
            [
                (start_hbm, start_ref),
                (stop_hbm, stop_ref),
                (twist_hbm, twist_ref),
                (bins_hbm, bins_ref),
                (inner_hbm, inner),
                (pool_hbm, pool_ref),
            ]
        )
    ]
    for table in tables_in:
        table.start()
    load.wait()
    packed[:, :full] = raw[0, :full].T
    packed[:, full : 2 * full] = raw[1, :full].T
    if tail:
        packed[:, 2 * full :] = jnp.concatenate([raw[0, full:], raw[1, full:]], axis=0).T
    pl.semaphore_wait(barrier, outer + 1)

    def rows_of(line, i):
        return pl.ds(pl.multiple_of(line * columns + begins[i], 8), sizes[i])

    def part(i):
        return pl.ds(begins[i], sizes[i])

    incoming = {}
    for i in range(chunks):
        for step in range(outer - 1, 0, -1):
            there = lax.rem(me + step, outer)
            incoming[i, step] = pltpu.make_async_remote_copy(
                src_ref=packed.at[rows_of(there, i)],
                dst_ref=gathered.at[me, part(i)],
                send_sem=in_send.at[i, step],
                recv_sem=in_recv.at[i, step],
                device_id={"line": there},
                device_id_type=MESH,
            )
            incoming[i, step].start()
    gathered[me] = packed[pl.ds(pl.multiple_of(me * columns, 8), columns), :]

    for table in tables_in:
        table.wait()
    lower = start_ref[date]
    upper = stop_ref[date]
    bins = bins_ref[...]
    keep = (bins >= lower) & (bins < upper)
    lane = lax.broadcasted_iota(jnp.int32, bins.shape, 2)
    imaginary = ((lane >= full) & (lane < 2 * full)) | (lane >= 2 * full + tail)
    keep_conj = jnp.where(keep, jnp.where(imaginary, -1.0, 1.0), 0.0).astype(jnp.float32)

    def inner_dft(values):
        high, low = split(values)
        dot = functools.partial(jnp.dot, preferred_element_type=jnp.float32)
        return dot(high, inner[0]) + (dot(low, inner[0]) + dot(high, inner[1]))

    samples = width // LOOKS
    lines_all = outer * width
    out_lane = lax.broadcasted_iota(jnp.int32, (1, 2 * samples), 1)
    scale = 1.0 / (lines_all * lines_all * LOOKS)
    out_scale = jnp.where(out_lane < samples, scale, -scale).astype(jnp.float32)

    handed, outgoing = {}, {}

    def forward(i):
        for step in range(1, outer):
            incoming[i, step].wait_recv()
        rows = short_dft([as_row(gathered[l, part(i), :], full, tail) for l in range(outer)])
        rows = [rows[0]] + [twisted(rows[k], twist_ref[k], full, tail) for k in range(1, outer)]
        result = inner_dft(jnp.concatenate([row.flat() for row in rows], axis=0))
        spectrum[:, part(i), :] = result.reshape(outer, sizes[i], 2 * width)
        handed[i] = pltpu.make_async_remote_copy(
            src_ref=spectrum.at[:, part(i)],
            dst_ref=partner.at[:, part(i)],
            send_sem=date_send.at[i],
            recv_sem=date_recv.at[i],
            device_id={"date": previous},
            device_id_type=MESH,
        )
        handed[i].start()

    def signal(values, chunk):
        rows = []
        for k in range(outer):
            row = as_row(values[k * chunk : (k + 1) * chunk], full, tail)
            rows.append(twisted(row, twist_ref[k], full, tail) if k else row)
        return short_dft(rows)

    def backward(i):
        handed[i].wait_recv()
        chunk = sizes[i]
        both = jnp.concatenate(
            [spectrum[:, part(i), :] * keep_conj, partner[:, part(i), :] * keep_conj], axis=0
        )
        both = inner_dft(both.reshape(2 * outer * chunk, 2 * width))
        ref = signal(both[: outer * chunk], chunk)
        sec = signal(both[outer * chunk :], chunk)
        product = jnp.concatenate([times_conj(r, s).flat() for r, s in zip(ref, sec)], axis=0)
        high, low = split(product)
        weights = pool_ref[...]
        means = jnp.dot(high, weights, preferred_element_type=jnp.float32)
        means = (means + jnp.dot(low, weights, preferred_element_type=jnp.float32)) * out_scale
        looked[:, part(i), :] = means.reshape(outer, chunk, 2 * samples)
        for step in range(1, outer):
            there = lax.rem(me + step, outer)
            outgoing[i, step] = pltpu.make_async_remote_copy(
                src_ref=looked.at[there, part(i)],
                dst_ref=landed.at[rows_of(me, i)],
                send_sem=out_send.at[i, step],
                recv_sem=out_recv.at[i, step],
                device_id={"line": there},
                device_id_type=MESH,
            )
            outgoing[i, step].start()
        landed[rows_of(me, i), :] = looked[me, part(i), :]

    for i in range(chunks + 1):
        if i < chunks:
            forward(i)
        if i >= 1:
            backward(i - 1)

    for copy in outgoing.values():
        copy.wait_recv()
    out_ref[0] = landed[...].T.reshape(2, samples, columns_all)
    for copies in (incoming, handed, outgoing):
        for copy in copies.values():
            copy.wait_send()


def shards(slc, band_start, band_stop):
    outer = lax.axis_size("line")
    _, _, columns_all, width = slc.shape
    columns = columns_all // outer
    chunks = len(chunk_sizes(columns))
    samples = width // LOOKS
    inner, twist, bins, pool = (jnp.asarray(t) for t in tables(outer, width))
    vmem = pl.BlockSpec(memory_space=pltpu.VMEM)
    hbm = pl.BlockSpec(memory_space=pltpu.HBM)
    f32 = jnp.float32
    dma = pltpu.SemaphoreType.DMA
    result = pl.pallas_call(
        kernel,
        out_shape=pltpu.VMEM((1, 2, samples, columns_all), f32),
        in_specs=[hbm, hbm, hbm, hbm, hbm, hbm, hbm],
        out_specs=vmem,
        scratch_shapes=[
            pltpu.VMEM((2, width, columns_all), f32),
            pltpu.VMEM((columns_all, 2 * width), f32),
            pltpu.VMEM(inner.shape, jnp.bfloat16),
            pltpu.VMEM(twist.shape, f32),
            pltpu.VMEM(bins.shape, jnp.int32),
            pltpu.VMEM(pool.shape, jnp.bfloat16),
            pltpu.SMEM(band_start.shape, jnp.int32),
            pltpu.SMEM(band_stop.shape, jnp.int32),
            pltpu.VMEM((outer, columns, 2 * width), f32),
            pltpu.VMEM((outer, columns, 2 * width), f32),
            pltpu.VMEM((outer, columns, 2 * width), f32),
            pltpu.VMEM((outer, columns, 2 * samples), f32),
            pltpu.VMEM((columns_all, 2 * samples), f32),
            dma,
            dma((6,)),
            dma((chunks, outer)),
            dma((chunks, outer)),
            dma((chunks,)),
            dma((chunks,)),
            dma((chunks, outer)),
            dma((chunks, outer)),
        ],
        compiler_params=pltpu.CompilerParams(
            collective_id=0, has_side_effects=True, vmem_limit_bytes=66000000
        ),
    )(jnp.swapaxes(slc, 2, 3), inner, twist, bins, pool, band_start, band_stop)
    return jnp.swapaxes(result, 2, 3)


def shared_kernel(
    slc_ref, inner_hbm, twist_hbm, bins_hbm, pool_hbm, start_hbm, stop_hbm, out_ref,
    raw, packed, inner, twist_ref, bins_ref, pool_ref, start_ref, stop_ref, gathered, ref_signal, sec_signal, looked, landed,
    load_sem, table_sem, in_send, in_recv, out_send, out_recv, from_below, from_above,
):
    outer = lax.axis_size("line")
    dates = lax.axis_size("date")
    me = lax.axis_index("line")
    date = lax.axis_index("date")
    width, columns_all = raw.shape[1], raw.shape[2]
    columns = columns_all // (outer * dates)
    full, tail, _, _ = layout(width)
    slots = slot_dates(dates)
    def at_date(relative):
        return lax.rem(date + relative, dates)

    def at_line(step):
        return lax.rem(me + step, outer)

    odd = lax.rem(date, 2)

    def slot_date(k):
        if k > 1 or dates == 2:
            return slots[k]
        return slots[k] + odd * (slots[1 - k] - slots[k])

    def device(relative, step):
        return {"date": at_date(relative), "line": at_line(step)}

    lower = me < outer // 2
    upper = me >= outer // 2
    partner = slot_date(0)

    barrier = pltpu.get_barrier_semaphore()
    for near, step in ((me > 0, outer - 1), (me < outer - 1, 1)):

        @pl.when(near)
        def _():
            for relative in (0, partner):
                pl.semaphore_signal(
                    barrier, inc=1, device_id=device(relative, step), device_id_type=MESH
                )

    for relative in range(1, dates):
        pl.semaphore_signal(barrier, inc=1, device_id=device(relative, 0), device_id_type=MESH)

    def tell(stage):
        @pl.when((me > 0) & (me + stage < outer))
        def _():
            pl.semaphore_signal(
                from_above.at[stage], inc=1, device_id={"line": me - 1}, device_id_type=MESH
            )

        @pl.when((me < outer - 1) & (me >= stage))
        def _():
            pl.semaphore_signal(
                from_below.at[stage], inc=1, device_id={"line": me + 1}, device_id_type=MESH
            )

    def hear(stage):
        @pl.when(me + stage + 1 < outer)
        def _():
            pl.semaphore_wait(from_above.at[stage], 1)

        @pl.when(me >= stage + 1)
        def _():
            pl.semaphore_wait(from_below.at[stage], 1)

    load = pltpu.make_async_copy(slc_ref.at[0], raw, load_sem)
    load.start()
    sides = (me > 0).astype(jnp.int32) + (me < outer - 1).astype(jnp.int32)
    pl.semaphore_wait(barrier, dates - 1 + 2 * sides)
    tell(0)
    tables_in = [
        pltpu.make_async_copy(source, target, table_sem.at[t])
        for t, (source, target) in enumerate(
            [
                (start_hbm, start_ref),
                (stop_hbm, stop_ref),
                (twist_hbm, twist_ref),
                (bins_hbm, bins_ref),
                (inner_hbm, inner),
                (pool_hbm, pool_ref),
            ]
        )
    ]
    load.wait()
    for table in tables_in:
        table.start()
    packed[:, :full] = raw[0, :full].T
    packed[:, full : 2 * full] = raw[1, :full].T
    if tail:
        packed[:, 2 * full :] = jnp.concatenate([raw[0, full:], raw[1, full:]], axis=0).T


    def rows_of(at, line):
        return pl.ds(pl.multiple_of((at * outer + line) * columns, 8), columns)

    incoming = {}
    for k in range(len(slots)):
        to = slot_date(k) if k < 2 else (dates - slots[k]) % dates
        for step in range(outer):
            if slots[k] or step:
                incoming[k, step] = pltpu.make_async_remote_copy(
                    src_ref=packed.at[rows_of(at_date(to), at_line(step))],
                    dst_ref=gathered.at[k, me],
                    send_sem=in_send.at[k, step],
                    recv_sem=in_recv.at[k, step],
                    device_id=device(to, step),
                    device_id_type=MESH,
                )

    sent = {}

    def send_in(k, step, known):
        if (k, step) not in incoming:
            return
        before = sent.get((k, step))
        sent[k, step] = known if before is None or known is None else before | known
        if before is not None:
            known = jnp.logical_not(before) if known is None else known & jnp.logical_not(before)
        if known is None:
            incoming[k, step].start()
        else:
            pl.when(known)(incoming[k, step].start)

    def distance(step):
        there = at_line(step)
        return jnp.maximum(there - me, me - there)

    def send_known(stage, ks):
        for k in ks:
            for step in range(outer - 1, -1, -1):
                near = stage + 2 if k in (0, len(slots) - 1) else stage + 1
                send_in(k, step, distance(step) <= near)

    for step, side in ((1, lower), (outer - 1, upper)):
        send_in(0, step, side)
    hear(0)
    send_known(0, [0])
    for stage in range(1, outer - 1):
        tell(stage)
        hear(stage)
    for k in range(len(slots)):
        for step in range(outer - 1, -1, -1):
            send_in(k, step, None)
    gathered[slots.index(0), me] = packed[rows_of(date, me), :]

    for table in tables_in:
        table.wait()
    bins = bins_ref[...]
    lane = lax.broadcasted_iota(jnp.int32, bins.shape, 2)
    imaginary = ((lane >= full) & (lane < 2 * full)) | (lane >= 2 * full + tail)
    sign = jnp.where(imaginary, -1.0, 1.0).astype(jnp.float32)

    def keep_conj(relative):
        pair = at_date(relative)
        return jnp.where((bins >= start_ref[pair]) & (bins < stop_ref[pair]), sign, 0.0)

    def inner_dft(values):
        high, low = split(values)
        count = values.shape[0]
        both = jnp.dot(jnp.concatenate([high, low], axis=0), inner[0], preferred_element_type=jnp.float32)
        return both[:count] + (both[count:] + jnp.dot(high, inner[1], preferred_element_type=jnp.float32))

    samples = width // LOOKS
    lines_all = outer * width
    out_lane = lax.broadcasted_iota(jnp.int32, (1, 2 * samples), 1)
    scale = 1.0 / (lines_all * lines_all * LOOKS)
    out_scale = jnp.where(out_lane < samples, scale, -scale).astype(jnp.float32)

    def filtered(k):
        relative = slot_date(k)
        before = lax.rem(relative + dates - 1, dates)
        lines = short_dft([as_row(gathered[k, l], full, tail) for l in range(outer)])
        lines = [lines[0]] + [twisted(lines[n], twist_ref[n], full, tail) for n in range(1, outer)]
        spectrum = inner_dft(jnp.concatenate([line.flat() for line in lines], axis=0))
        spectrum = spectrum.reshape(outer, columns, 2 * width)
        both = jnp.concatenate([spectrum * keep_conj(relative), spectrum * keep_conj(before)], axis=0)
        both = inner_dft(both.reshape(2 * outer * columns, 2 * width))
        both = both.reshape(2 * outer, columns, 2 * width)
        for base, target, pair in ((0, ref_signal, relative), (outer, sec_signal, before)):
            lines = []
            for n in range(outer):
                line = as_row(both[base + n], full, tail)
                lines.append(twisted(line, twist_ref[n], full, tail) if n else line)
            for n, line in enumerate(short_dft(lines)):
                target[pair, n] = line.flat()

    def multilook(pair):
        product = [
            times_conj(
                as_row(ref_signal[pair, n], full, tail), as_row(sec_signal[pair, n], full, tail)
            ).flat()
            for n in range(outer)
        ]
        high, low = split(jnp.concatenate(product, axis=0))
        means = jnp.dot(jnp.concatenate([high, low], axis=0), pool_ref[...], preferred_element_type=jnp.float32)
        means = (means[: outer * columns] + means[outer * columns :]) * out_scale
        looked[pair] = means.reshape(outer, columns, 2 * samples)

    outgoing = {}

    def send_out(pair):
        for step in [*range(1, outer), 0]:
            if pair == 0 and step == 0:
                landed[rows_of(date, me), :] = looked[0, me]
                continue
            outgoing[pair, step] = pltpu.make_async_remote_copy(
                src_ref=looked.at[pair, at_line(step)],
                dst_ref=landed.at[rows_of(date, me)],
                send_sem=out_send.at[pair, step],
                recv_sem=out_recv.at[pair, step],
                device_id=device(pair, step),
                device_id_type=MESH,
            )
            outgoing[pair, step].start()

    def ready(k):
        have = slots[: k + 1]
        pairs = {slots[k], (slots[k] + dates - 1) % dates}
        return sorted((p for p in pairs if p in have and (p + 1) % dates in have), key=lambda p: p == 0)

    held = []
    for k in range(len(slots)):
        for step in range(outer):
            if (k, step) in incoming:
                incoming[k, step].wait_recv()
        final = k == len(slots) - 1
        if final:
            for pair in held:
                send_out(pair)
        filtered(k)
        for pair in ready(k):
            multilook(pair)
            if final:
                send_out(pair)
            else:
                held.append(pair)

    for copy in outgoing.values():
        copy.wait_recv()
    out_ref[0] = landed[...].T.reshape(2, samples, columns_all)
    for copies in (incoming, outgoing):
        for copy in copies.values():
            copy.wait_send()


def slot_dates(dates):
    return list(range(1, dates, 2)) + list(range(2, dates, 2)) + [0]


def shared_shards(slc, band_start, band_stop):
    outer = lax.axis_size("line")
    dates = lax.axis_size("date")
    _, _, columns_all, width = slc.shape
    columns = columns_all // (outer * dates)
    samples = width // LOOKS
    inner, twist, bins, pool = (jnp.asarray(t) for t in tables(outer, width))
    vmem = pl.BlockSpec(memory_space=pltpu.VMEM)
    hbm = pl.BlockSpec(memory_space=pltpu.HBM)
    f32 = jnp.float32
    dma = pltpu.SemaphoreType.DMA
    result = pl.pallas_call(
        shared_kernel,
        out_shape=pltpu.VMEM((1, 2, samples, columns_all), f32),
        in_specs=[hbm, hbm, hbm, hbm, hbm, hbm, hbm],
        out_specs=vmem,
        scratch_shapes=[
            pltpu.VMEM((2, width, columns_all), f32),
            pltpu.VMEM((columns_all, 2 * width), f32),
            pltpu.VMEM(inner.shape, jnp.bfloat16),
            pltpu.VMEM(twist.shape, f32),
            pltpu.VMEM(bins.shape, jnp.int32),
            pltpu.VMEM(pool.shape, jnp.bfloat16),
            pltpu.SMEM(band_start.shape, jnp.int32),
            pltpu.SMEM(band_stop.shape, jnp.int32),
            pltpu.VMEM((dates, outer, columns, 2 * width), f32),
            pltpu.VMEM((dates, outer, columns, 2 * width), f32),
            pltpu.VMEM((dates, outer, columns, 2 * width), f32),
            pltpu.VMEM((dates, outer, columns, 2 * samples), f32),
            pltpu.VMEM((columns_all, 2 * samples), f32),
            dma,
            dma((6,)),
            dma((dates, outer)),
            dma((dates, outer)),
            dma((dates, outer)),
            dma((dates, outer)),
            pltpu.SemaphoreType.REGULAR((outer,)),
            pltpu.SemaphoreType.REGULAR((outer,)),
        ],
        compiler_params=pltpu.CompilerParams(
            collective_id=0, has_side_effects=True, vmem_limit_bytes=66000000
        ),
    )(jnp.swapaxes(slc, 2, 3), inner, twist, bins, pool, band_start, band_stop)
    return jnp.swapaxes(result, 2, 3)


def solution(mesh):
    group = mesh.shape["line"] * mesh.shape["date"]

    def body(slc, band_start, band_stop):
        shared = slc.shape[2] % (8 * group) == 0 and group > 1 and mesh.shape["date"] % 2 == 0
        return (shared_shards if shared else shards)(slc, band_start, band_stop)

    return jax.shard_map(
        body,
        mesh=mesh,
        in_specs=(P("date", None, "stack", "line"), P(), P()),
        out_specs=P("date", None, "stack", "line"),
        check_vma=False,
    )
```

```python
import functools

import jax
import jax.numpy as jnp
import numpy as np
from jax import lax
from jax.experimental import pallas as pl
from jax.experimental.pallas import tpu as pltpu
from jax.sharding import PartitionSpec as P

LOOKS = 5
LANES = 128
MESH = pl.DeviceIdType.MESH
CHUNK = 16
SMALL = 16


def layout(width):
    full = width // LANES * LANES
    tail = width - full
    assert 2 * tail in (0, LANES)
    comp = np.concatenate([np.zeros(full), np.ones(full), np.zeros(tail), np.ones(tail)])
    index = np.concatenate([np.arange(full), np.arange(full), np.arange(tail) + full, np.arange(tail) + full])
    return full, tail, comp.astype(np.int64), index.astype(np.int64)


def split(values):
    high = values.astype(jnp.bfloat16)
    return high, (values - high.astype(jnp.float32)).astype(jnp.bfloat16)


def tables(outer, width):
    full, tail, comp, index = layout(width)
    angle = 2.0 * np.pi / width * (index[:, None] * index[None, :] % width)
    c, s = np.cos(angle), np.sin(angle)
    same = comp[:, None] == comp[None, :]
    to_re = (comp[:, None] == 1) & (comp[None, :] == 0)
    dense = np.where(same, c, np.where(to_re, s, -s)).astype(np.float32)
    high = dense.astype(jnp.bfloat16)
    low = (dense - high.astype(np.float32)).astype(jnp.bfloat16)
    inner = np.stack([high, low])
    lines = outer * width
    turn = 2.0 * np.pi / lines * (np.arange(outer)[:, None] * index[None, :] % lines)
    along = np.cos(turn)
    across = np.where(comp[None, :] == 0, np.sin(turn), -np.sin(turn))
    twist = np.stack([along, across], axis=1).astype(np.float32)
    bins = (np.arange(outer)[:, None] + outer * index[None, :]).astype(np.int32)[:, None, :]
    samples = width // LOOKS
    target = index // LOOKS + samples * comp
    pool = (target[:, None] == np.arange(2 * samples)[None, :]).astype(jnp.bfloat16)
    return inner, twist, bins, pool


def chunk_sizes(columns):
    sizes, left = [], columns
    while left > CHUNK and left % SMALL == 0:
        sizes.append(CHUNK)
        left -= CHUNK
    if left % SMALL == 0:
        return sizes + [SMALL] * (left // SMALL)
    return sizes + [left]


class Row:
    def __init__(self, re, im, tail):
        self.re, self.im, self.tail = re, im, tail

    def __add__(self, other):
        return Row(self.re + other.re, self.im + other.im, None if self.tail is None else self.tail + other.tail)

    def __sub__(self, other):
        return Row(self.re - other.re, self.im - other.im, None if self.tail is None else self.tail - other.tail)

    def flat(self):
        parts = [self.re, self.im] + ([] if self.tail is None else [self.tail])
        return jnp.concatenate(parts, axis=-1)


def as_row(values, full, tail):
    return Row(
        values[:, :full],
        values[:, full : 2 * full],
        values[:, 2 * full :] if tail else None,
    )


def swapped(tail_values):
    return pltpu.roll(tail_values, LANES // 2, 1)


def first_half(tail_values):
    return lax.broadcasted_iota(jnp.int32, tail_values.shape, 1) < LANES // 2


def times_minus_i(row):
    tail = row.tail
    if tail is not None:
        turned = swapped(tail)
        tail = jnp.where(first_half(tail), turned, -turned)
    return Row(row.im, -row.re, tail)


def times_phase(row, c, s):
    tail = row.tail
    if tail is not None:
        turned = swapped(tail) * s
        tail = tail * c + jnp.where(first_half(tail), turned, -turned)
    return Row(row.re * c + row.im * s, row.im * c - row.re * s, tail)


def short_dft(rows):
    count = len(rows)
    if count == 1:
        return rows
    if count % 2:
        result = []
        for k in range(count):
            total = rows[0]
            for n in range(1, count):
                angle = 2.0 * np.pi * (n * k % count) / count
                total = total + times_phase(rows[n], float(np.cos(angle)), float(np.sin(angle)))
            result.append(total)
        return result
    even, odd = short_dft(rows[0::2]), short_dft(rows[1::2])
    half = count // 2
    low, high = [], []
    for k in range(half):
        if k == 0:
            turned = odd[k]
        elif 4 * k == count:
            turned = times_minus_i(odd[k])
        else:
            angle = 2.0 * np.pi * k / count
            turned = times_phase(odd[k], float(np.cos(angle)), float(np.sin(angle)))
        low.append(even[k] + turned)
        high.append(even[k] - turned)
    return low + high


def twisted(row, twist, full, tail):
    along, across = twist[0:1, :], twist[1:2, :]
    tail_values = row.tail
    if tail_values is not None:
        tail_values = tail_values * along[:, 2 * full :] + swapped(tail_values) * across[:, 2 * full :]
    return Row(
        row.re * along[:, :full] + row.im * across[:, :full],
        row.im * along[:, :full] + row.re * across[:, full : 2 * full],
        tail_values,
    )


def times_conj(ref, sec):
    tail = None
    if ref.tail is not None:
        straight = ref.tail * sec.tail
        crossed = ref.tail * swapped(sec.tail)
        tail = jnp.where(
            first_half(straight), straight + swapped(straight), crossed - swapped(crossed)
        )
    return Row(
        ref.re * sec.re + ref.im * sec.im,
        ref.im * sec.re - ref.re * sec.im,
        tail,
    )


def kernel(
    slc_ref, inner_hbm, twist_hbm, bins_hbm, pool_hbm, start_hbm, stop_hbm, out_ref,
    raw, packed, inner, twist_ref, bins_ref, pool_ref, start_ref, stop_ref, gathered, spectrum, partner, looked, landed,
    load_sem, table_sem, in_send, in_recv, date_send, date_recv, out_send, out_recv,
):
    outer = lax.axis_size("line")
    dates = lax.axis_size("date")
    me = lax.axis_index("line")
    date = lax.axis_index("date")
    width, columns_all = raw.shape[1], raw.shape[2]
    columns = columns_all // outer
    sizes = chunk_sizes(columns)
    chunks = len(sizes)
    begins = [sum(sizes[:i]) for i in range(chunks)]
    full, tail, _, _ = layout(width)
    previous = lax.rem(date + dates - 1, dates)
    following = lax.rem(date + 1, dates)

    barrier = pltpu.get_barrier_semaphore()
    for step in range(1, outer):
        pl.semaphore_signal(
            barrier, inc=1, device_id={"line": lax.rem(me + step, outer)}, device_id_type=MESH
        )
    for other in (previous, following):
        pl.semaphore_signal(barrier, inc=1, device_id={"date": other}, device_id_type=MESH)

    load = pltpu.make_async_copy(slc_ref.at[0], raw, load_sem)
    load.start()
    tables_in = [
        pltpu.make_async_copy(source, target, table_sem.at[t])
        for t, (source, target) in enumerate(
            [
                (start_hbm, start_ref),
                (stop_hbm, stop_ref),
                (twist_hbm, twist_ref),
                (bins_hbm, bins_ref),
                (inner_hbm, inner),
                (pool_hbm, pool_ref),
            ]
        )
    ]
    for table in tables_in:
        table.start()
    load.wait()
    packed[:, :full] = raw[0, :full].T
    packed[:, full : 2 * full] = raw[1, :full].T
    if tail:
        packed[:, 2 * full :] = jnp.concatenate([raw[0, full:], raw[1, full:]], axis=0).T
    pl.semaphore_wait(barrier, outer + 1)

    def rows_of(line, i):
        return pl.ds(pl.multiple_of(line * columns + begins[i], 8), sizes[i])

    def part(i):
        return pl.ds(begins[i], sizes[i])

    incoming = {}
    for i in range(chunks):
        for step in range(outer - 1, 0, -1):
            there = lax.rem(me + step, outer)
            incoming[i, step] = pltpu.make_async_remote_copy(
                src_ref=packed.at[rows_of(there, i)],
                dst_ref=gathered.at[me, part(i)],
                send_sem=in_send.at[i, step],
                recv_sem=in_recv.at[i, step],
                device_id={"line": there},
                device_id_type=MESH,
            )
            incoming[i, step].start()
    gathered[me] = packed[pl.ds(pl.multiple_of(me * columns, 8), columns), :]

    for table in tables_in:
        table.wait()
    lower = start_ref[date]
    upper = stop_ref[date]
    bins = bins_ref[...]
    keep = (bins >= lower) & (bins < upper)
    lane = lax.broadcasted_iota(jnp.int32, bins.shape, 2)
    imaginary = ((lane >= full) & (lane < 2 * full)) | (lane >= 2 * full + tail)
    keep_conj = jnp.where(keep, jnp.where(imaginary, -1.0, 1.0), 0.0).astype(jnp.float32)

    def inner_dft(values):
        high, low = split(values)
        dot = functools.partial(jnp.dot, preferred_element_type=jnp.float32)
        return dot(high, inner[0]) + (dot(low, inner[0]) + dot(high, inner[1]))

    samples = width // LOOKS
    lines_all = outer * width
    out_lane = lax.broadcasted_iota(jnp.int32, (1, 2 * samples), 1)
    scale = 1.0 / (lines_all * lines_all * LOOKS)
    out_scale = jnp.where(out_lane < samples, scale, -scale).astype(jnp.float32)

    handed, outgoing = {}, {}

    def forward(i):
        for step in range(1, outer):
            incoming[i, step].wait_recv()
        rows = short_dft([as_row(gathered[l, part(i), :], full, tail) for l in range(outer)])
        rows = [rows[0]] + [twisted(rows[k], twist_ref[k], full, tail) for k in range(1, outer)]
        result = inner_dft(jnp.concatenate([row.flat() for row in rows], axis=0))
        spectrum[:, part(i), :] = result.reshape(outer, sizes[i], 2 * width)
        handed[i] = pltpu.make_async_remote_copy(
            src_ref=spectrum.at[:, part(i)],
            dst_ref=partner.at[:, part(i)],
            send_sem=date_send.at[i],
            recv_sem=date_recv.at[i],
            device_id={"date": previous},
            device_id_type=MESH,
        )
        handed[i].start()

    def signal(values, chunk):
        rows = []
        for k in range(outer):
            row = as_row(values[k * chunk : (k + 1) * chunk], full, tail)
            rows.append(twisted(row, twist_ref[k], full, tail) if k else row)
        return short_dft(rows)

    def backward(i):
        handed[i].wait_recv()
        chunk = sizes[i]
        both = jnp.concatenate(
            [spectrum[:, part(i), :] * keep_conj, partner[:, part(i), :] * keep_conj], axis=0
        )
        both = inner_dft(both.reshape(2 * outer * chunk, 2 * width))
        ref = signal(both[: outer * chunk], chunk)
        sec = signal(both[outer * chunk :], chunk)
        product = jnp.concatenate([times_conj(r, s).flat() for r, s in zip(ref, sec)], axis=0)
        high, low = split(product)
        weights = pool_ref[...]
        means = jnp.dot(high, weights, preferred_element_type=jnp.float32)
        means = (means + jnp.dot(low, weights, preferred_element_type=jnp.float32)) * out_scale
        looked[:, part(i), :] = means.reshape(outer, chunk, 2 * samples)
        for step in range(1, outer):
            there = lax.rem(me + step, outer)
            outgoing[i, step] = pltpu.make_async_remote_copy(
                src_ref=looked.at[there, part(i)],
                dst_ref=landed.at[rows_of(me, i)],
                send_sem=out_send.at[i, step],
                recv_sem=out_recv.at[i, step],
                device_id={"line": there},
                device_id_type=MESH,
            )
            outgoing[i, step].start()
        landed[rows_of(me, i), :] = looked[me, part(i), :]

    for i in range(chunks + 1):
        if i < chunks:
            forward(i)
        if i >= 1:
            backward(i - 1)

    for copy in outgoing.values():
        copy.wait_recv()
    out_ref[0] = landed[...].T.reshape(2, samples, columns_all)
    for copies in (incoming, handed, outgoing):
        for copy in copies.values():
            copy.wait_send()


def shards(slc, band_start, band_stop):
    outer = lax.axis_size("line")
    _, _, columns_all, width = slc.shape
    columns = columns_all // outer
    chunks = len(chunk_sizes(columns))
    samples = width // LOOKS
    inner, twist, bins, pool = (jnp.asarray(t) for t in tables(outer, width))
    vmem = pl.BlockSpec(memory_space=pltpu.VMEM)
    hbm = pl.BlockSpec(memory_space=pltpu.HBM)
    f32 = jnp.float32
    dma = pltpu.SemaphoreType.DMA
    result = pl.pallas_call(
        kernel,
        out_shape=pltpu.VMEM((1, 2, samples, columns_all), f32),
        in_specs=[hbm, hbm, hbm, hbm, hbm, hbm, hbm],
        out_specs=vmem,
        scratch_shapes=[
            pltpu.VMEM((2, width, columns_all), f32),
            pltpu.VMEM((columns_all, 2 * width), f32),
            pltpu.VMEM(inner.shape, jnp.bfloat16),
            pltpu.VMEM(twist.shape, f32),
            pltpu.VMEM(bins.shape, jnp.int32),
            pltpu.VMEM(pool.shape, jnp.bfloat16),
            pltpu.SMEM(band_start.shape, jnp.int32),
            pltpu.SMEM(band_stop.shape, jnp.int32),
            pltpu.VMEM((outer, columns, 2 * width), f32),
            pltpu.VMEM((outer, columns, 2 * width), f32),
            pltpu.VMEM((outer, columns, 2 * width), f32),
            pltpu.VMEM((outer, columns, 2 * samples), f32),
            pltpu.VMEM((columns_all, 2 * samples), f32),
            dma,
            dma((6,)),
            dma((chunks, outer)),
            dma((chunks, outer)),
            dma((chunks,)),
            dma((chunks,)),
            dma((chunks, outer)),
            dma((chunks, outer)),
        ],
        compiler_params=pltpu.CompilerParams(
            collective_id=0, has_side_effects=True, vmem_limit_bytes=66000000
        ),
    )(jnp.swapaxes(slc, 2, 3), inner, twist, bins, pool, band_start, band_stop)
    return jnp.swapaxes(result, 2, 3)


def shared_tables(outer, width):
    block = LANES // 2
    lines = outer * width
    count = lines // block
    index = np.arange(LANES) % block
    side = np.arange(LANES) // block
    angle = 2.0 * np.pi / block * (index[:, None] * index[None, :] % block)
    same = side[:, None] == side[None, :]
    dense = np.concatenate([np.where(same, np.cos(angle), 0.0), np.where(same, np.sin(angle), 0.0)], axis=1)
    dense = dense.astype(np.float32)
    high = dense.astype(jnp.bfloat16)
    low = (dense - high.astype(np.float32)).astype(jnp.bfloat16)
    inner = np.concatenate([high, high, low], axis=0)
    turn = 2.0 * np.pi / lines * (np.arange(count)[:, None] * index[None, :] % lines)
    twist = np.stack([np.cos(turn), np.sin(turn)], axis=1).astype(np.float32)
    bins = (np.arange(count)[:, None] + count * index[None, :]).astype(np.int32)[:, None, :]
    samples = width // LOOKS
    line = np.arange(width // block)[:, None, None] * block + np.arange(block)[None, None, :]
    target = line // LOOKS + samples * np.arange(2)[None, :, None]
    pool = (target.reshape(-1)[:, None] == np.arange(2 * samples)[None, :]).astype(jnp.bfloat16)
    return inner, twist, bins, pool


def turned(value, c, s):
    re, im = value
    return re * c + im * s, im * c - re * s


def plus(a, b):
    return a[0] + b[0], a[1] + b[1]


def minus(a, b):
    return a[0] - b[0], a[1] - b[1]


def times(a, factor):
    return a[0] * factor, a[1] * factor


def full_dft(values):
    count = len(values)
    if count == 1:
        return values
    if count % 2:
        sums = [plus(values[j], values[count - j]) for j in range(1, count // 2 + 1)]
        differences = [minus(values[j], values[count - j]) for j in range(1, count // 2 + 1)]
        result = [None] * count
        result[0] = functools.reduce(plus, sums, values[0])
        for k in range(1, count // 2 + 1):
            angles = [2.0 * np.pi * (j * k % count) / count for j in range(1, count // 2 + 1)]
            even = functools.reduce(plus, [times(v, float(np.cos(a))) for v, a in zip(sums, angles)], values[0])
            odd = functools.reduce(plus, [times(v, float(np.sin(a))) for v, a in zip(differences, angles)])
            result[k] = even[0] + odd[1], even[1] - odd[0]
            result[count - k] = even[0] - odd[1], even[1] + odd[0]
        return result
    even, odd = full_dft(values[0::2]), full_dft(values[1::2])
    low, high = [], []
    for k in range(count // 2):
        if k == 0:
            moved = odd[k]
        elif 4 * k == count:
            moved = odd[k][1], -odd[k][0]
        else:
            angle = 2.0 * np.pi * k / count
            moved = turned(odd[k], float(np.cos(angle)), float(np.sin(angle)))
        low.append(plus(even[k], moved))
        high.append(minus(even[k], moved))
    return low + high


def shared_kernel(
    slc_ref, inner_hbm, twist_hbm, bins_hbm, pool_hbm, start_hbm, stop_hbm, out_ref,
    raw, packed, inner, twist_ref, bins_ref, pool_ref, start_ref, stop_ref, gathered, ref_signal, sec_signal, looked, landed,
    load_sem, table_sem, in_send, in_recv, out_send, out_recv, from_below, from_above,
):
    outer = lax.axis_size("line")
    dates = lax.axis_size("date")
    me = lax.axis_index("line")
    date = lax.axis_index("date")
    width, columns_all = raw.shape[1], raw.shape[2]
    half = columns_all // 2
    rows = half // (outer * dates)
    block = LANES // 2
    blocks = width // block
    count = outer * blocks
    flat = 2 * width
    slots = slot_dates(dates)
    def at_date(relative):
        return lax.rem(date + relative, dates)

    def at_line(step):
        return lax.rem(me + step, outer)

    odd = lax.rem(date, 2)

    def slot_date(k):
        if k > 1 or dates == 2:
            return slots[k]
        return slots[k] + odd * (slots[1 - k] - slots[k])

    def device(relative, step):
        return {"date": at_date(relative), "line": at_line(step)}

    lower = me < outer // 2
    upper = me >= outer // 2
    partner = slot_date(0)

    barrier = pltpu.get_barrier_semaphore()
    for near, step in ((me > 0, outer - 1), (me < outer - 1, 1)):

        @pl.when(near)
        def _():
            for relative in (0, partner):
                pl.semaphore_signal(
                    barrier, inc=1, device_id=device(relative, step), device_id_type=MESH
                )

    for relative in range(1, dates):
        pl.semaphore_signal(barrier, inc=1, device_id=device(relative, 0), device_id_type=MESH)

    def tell(stage):
        @pl.when((me > 0) & (me + stage < outer))
        def _():
            pl.semaphore_signal(
                from_above.at[stage], inc=1, device_id={"line": me - 1}, device_id_type=MESH
            )

        @pl.when((me < outer - 1) & (me >= stage))
        def _():
            pl.semaphore_signal(
                from_below.at[stage], inc=1, device_id={"line": me + 1}, device_id_type=MESH
            )

    def hear(stage):
        @pl.when(me + stage + 1 < outer)
        def _():
            pl.semaphore_wait(from_above.at[stage], 1)

        @pl.when(me >= stage + 1)
        def _():
            pl.semaphore_wait(from_below.at[stage], 1)

    load = pltpu.make_async_copy(slc_ref.at[0], raw, load_sem)
    load.start()
    sides = (me > 0).astype(jnp.int32) + (me < outer - 1).astype(jnp.int32)
    pl.semaphore_wait(barrier, dates - 1 + 2 * sides)
    tell(0)
    tables_in = [
        pltpu.make_async_copy(source, target, table_sem.at[t])
        for t, (source, target) in enumerate(
            [
                (start_hbm, start_ref),
                (stop_hbm, stop_ref),
                (twist_hbm, twist_ref),
                (bins_hbm, bins_ref),
                (inner_hbm, inner),
                (pool_hbm, pool_ref),
            ]
        )
    ]
    load.wait()
    for table in tables_in:
        table.start()
    for part in range(2):
        for n in range(blocks):
            lines = raw[part, n * block : (n + 1) * block]
            both = jnp.concatenate([lines[:, :half], lines[:, half:]], axis=0)
            packed[:, part * flat + n * LANES : part * flat + (n + 1) * LANES] = both.T

    def rows_of(at, line):
        return pl.ds(pl.multiple_of((at * outer + line) * rows, 8), rows)

    incoming = {}
    for k in range(len(slots)):
        to = slot_date(k) if k < 2 else (dates - slots[k]) % dates
        for step in range(outer):
            if slots[k] or step:
                incoming[k, step] = pltpu.make_async_remote_copy(
                    src_ref=packed.at[rows_of(at_date(to), at_line(step))],
                    dst_ref=gathered.at[k, me],
                    send_sem=in_send.at[k, step],
                    recv_sem=in_recv.at[k, step],
                    device_id=device(to, step),
                    device_id_type=MESH,
                )

    sent = {}

    def send_in(k, step, known):
        if (k, step) not in incoming:
            return
        before = sent.get((k, step))
        sent[k, step] = known if before is None or known is None else before | known
        if before is not None:
            known = jnp.logical_not(before) if known is None else known & jnp.logical_not(before)
        if known is None:
            incoming[k, step].start()
        else:
            pl.when(known)(incoming[k, step].start)

    def distance(step):
        there = at_line(step)
        return jnp.maximum(there - me, me - there)

    def send_known(stage, ks):
        for k in ks:
            for step in range(outer - 1, -1, -1):
                near = stage + 2 if k in (0, len(slots) - 1) else stage + 1
                send_in(k, step, distance(step) <= near)

    for step, side in ((1, lower), (outer - 1, upper)):
        send_in(0, step, side)
    hear(0)
    send_known(0, [0])
    for stage in range(1, outer - 1):
        tell(stage)
        hear(stage)
    for k in range(len(slots)):
        for step in range(outer - 1, -1, -1):
            send_in(k, step, None)
    gathered[slots.index(0), me] = packed[rows_of(date, me), :]

    for table in tables_in:
        table.wait()
    bins = bins_ref[...]

    def kept(relative):
        pair = at_date(relative)
        return jnp.where((bins >= start_ref[pair]) & (bins < stop_ref[pair]), 1.0, 0.0).astype(jnp.float32)

    def inner_dft(re, im):
        values = jnp.concatenate([re, im], axis=0)
        high, low = split(values)
        both = jnp.dot(
            jnp.concatenate([high, low, high], axis=1), inner[...], preferred_element_type=jnp.float32
        )
        size = re.shape[0]
        return (
            both[:size, :LANES] + both[size:, LANES:],
            both[size:, :LANES] - both[:size, LANES:],
        )

    def twisted_by(values):
        return [values[0]] + [
            turned(values[n], twist_ref[n, 0:1, :], twist_ref[n, 1:2, :]) for n in range(1, len(values))
        ]

    samples = width // LOOKS
    lines_all = outer * width
    scale = 1.0 / (lines_all * lines_all * LOOKS)

    def lanes(part, n):
        return slice(part * flat + n * LANES, part * flat + (n + 1) * LANES)

    def filtered(k):
        relative = slot_date(k)
        before = lax.rem(relative + dates - 1, dates)
        values = [
            (gathered[k, l, :, lanes(0, n)], gathered[k, l, :, lanes(1, n)])
            for l in range(outer)
            for n in range(blocks)
        ]
        values = twisted_by(full_dft(values))
        re, im = inner_dft(
            jnp.concatenate([v[0] for v in values], axis=0), jnp.concatenate([v[1] for v in values], axis=0)
        )
        re, im = re.reshape(count, rows, LANES), im.reshape(count, rows, LANES)
        keeps = [kept(relative), kept(before)]
        re = jnp.concatenate([re * keep for keep in keeps], axis=0).reshape(2 * count * rows, LANES)
        im = jnp.concatenate([im * -keep for keep in keeps], axis=0).reshape(2 * count * rows, LANES)
        re, im = inner_dft(re, im)
        for base, target, pair in ((0, ref_signal, relative), (count, sec_signal, before)):
            values = [
                (re[(base + n) * rows : (base + n + 1) * rows], im[(base + n) * rows : (base + n + 1) * rows])
                for n in range(count)
            ]
            values = full_dft(twisted_by(values))
            for n, value in enumerate(values):
                for part in range(2):
                    target[pair, n // blocks, :, lanes(part, n % blocks)] = value[part]

    def multilook(pair):
        re, im = [], []
        for l in range(outer):
            ref_re, ref_im = ref_signal[pair, l, :, :flat], ref_signal[pair, l, :, flat:]
            sec_re, sec_im = sec_signal[pair, l, :, :flat], sec_signal[pair, l, :, flat:]
            re.append(ref_re * sec_re + ref_im * sec_im)
            im.append(ref_im * sec_re - ref_re * sec_im)
        high, low = split(jnp.concatenate(re + im, axis=0))
        means = jnp.dot(jnp.concatenate([high, low], axis=0), pool_ref[...], preferred_element_type=jnp.float32)
        size = outer * rows
        means = means[: 2 * size] + means[2 * size :]
        looked[pair, :, :, : 2 * samples] = (means[:size] * scale).reshape(outer, rows, 2 * samples)
        looked[pair, :, :, 2 * samples :] = (means[size:] * -scale).reshape(outer, rows, 2 * samples)

    outgoing = {}

    def send_out(pair):
        for step in [*range(1, outer), 0]:
            if pair == 0 and step == 0:
                landed[rows_of(date, me), :] = looked[0, me]
                continue
            outgoing[pair, step] = pltpu.make_async_remote_copy(
                src_ref=looked.at[pair, at_line(step)],
                dst_ref=landed.at[rows_of(date, me)],
                send_sem=out_send.at[pair, step],
                recv_sem=out_recv.at[pair, step],
                device_id=device(pair, step),
                device_id_type=MESH,
            )
            outgoing[pair, step].start()

    def ready(k):
        have = slots[: k + 1]
        pairs = {slots[k], (slots[k] + dates - 1) % dates}
        return sorted((p for p in pairs if p in have and (p + 1) % dates in have), key=lambda p: p == 0)

    held = []
    for k in range(len(slots)):
        for step in range(outer):
            if (k, step) in incoming:
                incoming[k, step].wait_recv()
        final = k == len(slots) - 1
        if final:
            for pair in held:
                send_out(pair)
        filtered(k)
        for pair in ready(k):
            multilook(pair)
            if final:
                send_out(pair)
            else:
                held.append(pair)

    for copy in outgoing.values():
        copy.wait_recv()
    for part in range(2):
        turned_back = landed[:, part * 2 * samples : (part + 1) * 2 * samples].T
        out_ref[0, part, :, :half] = turned_back[:samples]
        out_ref[0, part, :, half:] = turned_back[samples:]
    for copies in (incoming, outgoing):
        for copy in copies.values():
            copy.wait_send()


def slot_dates(dates):
    return list(range(1, dates, 2)) + list(range(2, dates, 2)) + [0]


def shared_shards(slc, band_start, band_stop):
    outer = lax.axis_size("line")
    dates = lax.axis_size("date")
    _, _, columns_all, width = slc.shape
    half = columns_all // 2
    rows = half // (outer * dates)
    samples = width // LOOKS
    inner, twist, bins, pool = (jnp.asarray(t) for t in shared_tables(outer, width))
    vmem = pl.BlockSpec(memory_space=pltpu.VMEM)
    hbm = pl.BlockSpec(memory_space=pltpu.HBM)
    f32 = jnp.float32
    dma = pltpu.SemaphoreType.DMA
    result = pl.pallas_call(
        shared_kernel,
        out_shape=pltpu.VMEM((1, 2, samples, columns_all), f32),
        in_specs=[hbm, hbm, hbm, hbm, hbm, hbm, hbm],
        out_specs=vmem,
        scratch_shapes=[
            pltpu.VMEM((2, width, columns_all), f32),
            pltpu.VMEM((half, 4 * width), f32),
            pltpu.VMEM(inner.shape, jnp.bfloat16),
            pltpu.VMEM(twist.shape, f32),
            pltpu.VMEM(bins.shape, jnp.int32),
            pltpu.VMEM(pool.shape, jnp.bfloat16),
            pltpu.SMEM(band_start.shape, jnp.int32),
            pltpu.SMEM(band_stop.shape, jnp.int32),
            pltpu.VMEM((dates, outer, rows, 4 * width), f32),
            pltpu.VMEM((dates, outer, rows, 4 * width), f32),
            pltpu.VMEM((dates, outer, rows, 4 * width), f32),
            pltpu.VMEM((dates, outer, rows, 4 * samples), f32),
            pltpu.VMEM((half, 4 * samples), f32),
            dma,
            dma((6,)),
            dma((dates, outer)),
            dma((dates, outer)),
            dma((dates, outer)),
            dma((dates, outer)),
            pltpu.SemaphoreType.REGULAR((outer,)),
            pltpu.SemaphoreType.REGULAR((outer,)),
        ],
        compiler_params=pltpu.CompilerParams(
            collective_id=0, has_side_effects=True, vmem_limit_bytes=66000000
        ),
    )(jnp.swapaxes(slc, 2, 3), inner, twist, bins, pool, band_start, band_stop)
    return jnp.swapaxes(result, 2, 3)


def solution(mesh):
    group = mesh.shape["line"] * mesh.shape["date"]

    def body(slc, band_start, band_stop):
        half, width = slc.shape[2] // 2, slc.shape[3]
        shared = half % (8 * group) == 0 and half % LANES == 0 and mesh.shape["date"] % 2 == 0
        shared = shared and width % LANES == LANES // 2 and 2 * (width // LOOKS) % LANES == 0
        return (shared_shards if shared else shards)(slc, band_start, band_stop)

    return jax.shard_map(
        body,
        mesh=mesh,
        in_specs=(P("date", None, "stack", "line"), P(), P()),
        out_specs=P("date", None, "stack", "line"),
        check_vma=False,
    )
```

```python
import functools

import jax
import jax.numpy as jnp
import numpy as np
from jax import lax
from jax.experimental import pallas as pl
from jax.experimental.pallas import tpu as pltpu
from jax.sharding import PartitionSpec as P

LOOKS = 5
LANES = 128
MESH = pl.DeviceIdType.MESH
CHUNK = 16
SMALL = 16


def layout(width):
    full = width // LANES * LANES
    tail = width - full
    assert 2 * tail in (0, LANES)
    comp = np.concatenate([np.zeros(full), np.ones(full), np.zeros(tail), np.ones(tail)])
    index = np.concatenate([np.arange(full), np.arange(full), np.arange(tail) + full, np.arange(tail) + full])
    return full, tail, comp.astype(np.int64), index.astype(np.int64)


def split(values):
    high = values.astype(jnp.bfloat16)
    return high, (values - high.astype(jnp.float32)).astype(jnp.bfloat16)


def tables(outer, width):
    full, tail, comp, index = layout(width)
    angle = 2.0 * np.pi / width * (index[:, None] * index[None, :] % width)
    c, s = np.cos(angle), np.sin(angle)
    same = comp[:, None] == comp[None, :]
    to_re = (comp[:, None] == 1) & (comp[None, :] == 0)
    dense = np.where(same, c, np.where(to_re, s, -s)).astype(np.float32)
    high = dense.astype(jnp.bfloat16)
    low = (dense - high.astype(np.float32)).astype(jnp.bfloat16)
    inner = np.stack([high, low])
    lines = outer * width
    turn = 2.0 * np.pi / lines * (np.arange(outer)[:, None] * index[None, :] % lines)
    along = np.cos(turn)
    across = np.where(comp[None, :] == 0, np.sin(turn), -np.sin(turn))
    twist = np.stack([along, across], axis=1).astype(np.float32)
    bins = (np.arange(outer)[:, None] + outer * index[None, :]).astype(np.int32)[:, None, :]
    samples = width // LOOKS
    target = index // LOOKS + samples * comp
    pool = (target[:, None] == np.arange(2 * samples)[None, :]).astype(jnp.bfloat16)
    return inner, twist, bins, pool


def chunk_sizes(columns):
    sizes, left = [], columns
    while left > CHUNK and left % SMALL == 0:
        sizes.append(CHUNK)
        left -= CHUNK
    if left % SMALL == 0:
        return sizes + [SMALL] * (left // SMALL)
    return sizes + [left]


class Row:
    def __init__(self, re, im, tail):
        self.re, self.im, self.tail = re, im, tail

    def __add__(self, other):
        return Row(self.re + other.re, self.im + other.im, None if self.tail is None else self.tail + other.tail)

    def __sub__(self, other):
        return Row(self.re - other.re, self.im - other.im, None if self.tail is None else self.tail - other.tail)

    def flat(self):
        parts = [self.re, self.im] + ([] if self.tail is None else [self.tail])
        return jnp.concatenate(parts, axis=-1)


def as_row(values, full, tail):
    return Row(
        values[:, :full],
        values[:, full : 2 * full],
        values[:, 2 * full :] if tail else None,
    )


def swapped(tail_values):
    return pltpu.roll(tail_values, LANES // 2, 1)


def first_half(tail_values):
    return lax.broadcasted_iota(jnp.int32, tail_values.shape, 1) < LANES // 2


def times_minus_i(row):
    tail = row.tail
    if tail is not None:
        turned = swapped(tail)
        tail = jnp.where(first_half(tail), turned, -turned)
    return Row(row.im, -row.re, tail)


def times_phase(row, c, s):
    tail = row.tail
    if tail is not None:
        turned = swapped(tail) * s
        tail = tail * c + jnp.where(first_half(tail), turned, -turned)
    return Row(row.re * c + row.im * s, row.im * c - row.re * s, tail)


def short_dft(rows):
    count = len(rows)
    if count == 1:
        return rows
    if count % 2:
        result = []
        for k in range(count):
            total = rows[0]
            for n in range(1, count):
                angle = 2.0 * np.pi * (n * k % count) / count
                total = total + times_phase(rows[n], float(np.cos(angle)), float(np.sin(angle)))
            result.append(total)
        return result
    even, odd = short_dft(rows[0::2]), short_dft(rows[1::2])
    half = count // 2
    low, high = [], []
    for k in range(half):
        if k == 0:
            turned = odd[k]
        elif 4 * k == count:
            turned = times_minus_i(odd[k])
        else:
            angle = 2.0 * np.pi * k / count
            turned = times_phase(odd[k], float(np.cos(angle)), float(np.sin(angle)))
        low.append(even[k] + turned)
        high.append(even[k] - turned)
    return low + high


def twisted(row, twist, full, tail):
    along, across = twist[0:1, :], twist[1:2, :]
    tail_values = row.tail
    if tail_values is not None:
        tail_values = tail_values * along[:, 2 * full :] + swapped(tail_values) * across[:, 2 * full :]
    return Row(
        row.re * along[:, :full] + row.im * across[:, :full],
        row.im * along[:, :full] + row.re * across[:, full : 2 * full],
        tail_values,
    )


def times_conj(ref, sec):
    tail = None
    if ref.tail is not None:
        straight = ref.tail * sec.tail
        crossed = ref.tail * swapped(sec.tail)
        tail = jnp.where(
            first_half(straight), straight + swapped(straight), crossed - swapped(crossed)
        )
    return Row(
        ref.re * sec.re + ref.im * sec.im,
        ref.im * sec.re - ref.re * sec.im,
        tail,
    )


def kernel(
    slc_ref, inner_hbm, twist_hbm, bins_hbm, pool_hbm, start_hbm, stop_hbm, out_ref,
    raw, packed, inner, twist_ref, bins_ref, pool_ref, start_ref, stop_ref, gathered, spectrum, partner, looked, landed,
    load_sem, table_sem, in_send, in_recv, date_send, date_recv, out_send, out_recv,
):
    outer = lax.axis_size("line")
    dates = lax.axis_size("date")
    me = lax.axis_index("line")
    date = lax.axis_index("date")
    width, columns_all = raw.shape[1], raw.shape[2]
    columns = columns_all // outer
    sizes = chunk_sizes(columns)
    chunks = len(sizes)
    begins = [sum(sizes[:i]) for i in range(chunks)]
    full, tail, _, _ = layout(width)
    previous = lax.rem(date + dates - 1, dates)
    following = lax.rem(date + 1, dates)

    barrier = pltpu.get_barrier_semaphore()
    for step in range(1, outer):
        pl.semaphore_signal(
            barrier, inc=1, device_id={"line": lax.rem(me + step, outer)}, device_id_type=MESH
        )
    for other in (previous, following):
        pl.semaphore_signal(barrier, inc=1, device_id={"date": other}, device_id_type=MESH)

    load = pltpu.make_async_copy(slc_ref.at[0], raw, load_sem)
    load.start()
    tables_in = [
        pltpu.make_async_copy(source, target, table_sem.at[t])
        for t, (source, target) in enumerate(
            [
                (start_hbm, start_ref),
                (stop_hbm, stop_ref),
                (twist_hbm, twist_ref),
                (bins_hbm, bins_ref),
                (inner_hbm, inner),
                (pool_hbm, pool_ref),
            ]
        )
    ]
    for table in tables_in:
        table.start()
    load.wait()
    packed[:, :full] = raw[0, :full].T
    packed[:, full : 2 * full] = raw[1, :full].T
    if tail:
        packed[:, 2 * full :] = jnp.concatenate([raw[0, full:], raw[1, full:]], axis=0).T
    pl.semaphore_wait(barrier, outer + 1)

    def rows_of(line, i):
        return pl.ds(pl.multiple_of(line * columns + begins[i], 8), sizes[i])

    def part(i):
        return pl.ds(begins[i], sizes[i])

    incoming = {}
    for i in range(chunks):
        for step in range(outer - 1, 0, -1):
            there = lax.rem(me + step, outer)
            incoming[i, step] = pltpu.make_async_remote_copy(
                src_ref=packed.at[rows_of(there, i)],
                dst_ref=gathered.at[me, part(i)],
                send_sem=in_send.at[i, step],
                recv_sem=in_recv.at[i, step],
                device_id={"line": there},
                device_id_type=MESH,
            )
            incoming[i, step].start()
    gathered[me] = packed[pl.ds(pl.multiple_of(me * columns, 8), columns), :]

    for table in tables_in:
        table.wait()
    lower = start_ref[date]
    upper = stop_ref[date]
    bins = bins_ref[...]
    keep = (bins >= lower) & (bins < upper)
    lane = lax.broadcasted_iota(jnp.int32, bins.shape, 2)
    imaginary = ((lane >= full) & (lane < 2 * full)) | (lane >= 2 * full + tail)
    keep_conj = jnp.where(keep, jnp.where(imaginary, -1.0, 1.0), 0.0).astype(jnp.float32)

    def inner_dft(values):
        high, low = split(values)
        dot = functools.partial(jnp.dot, preferred_element_type=jnp.float32)
        return dot(high, inner[0]) + (dot(low, inner[0]) + dot(high, inner[1]))

    samples = width // LOOKS
    lines_all = outer * width
    out_lane = lax.broadcasted_iota(jnp.int32, (1, 2 * samples), 1)
    scale = 1.0 / (lines_all * lines_all * LOOKS)
    out_scale = jnp.where(out_lane < samples, scale, -scale).astype(jnp.float32)

    handed, outgoing = {}, {}

    def forward(i):
        for step in range(1, outer):
            incoming[i, step].wait_recv()
        rows = short_dft([as_row(gathered[l, part(i), :], full, tail) for l in range(outer)])
        rows = [rows[0]] + [twisted(rows[k], twist_ref[k], full, tail) for k in range(1, outer)]
        result = inner_dft(jnp.concatenate([row.flat() for row in rows], axis=0))
        spectrum[:, part(i), :] = result.reshape(outer, sizes[i], 2 * width)
        handed[i] = pltpu.make_async_remote_copy(
            src_ref=spectrum.at[:, part(i)],
            dst_ref=partner.at[:, part(i)],
            send_sem=date_send.at[i],
            recv_sem=date_recv.at[i],
            device_id={"date": previous},
            device_id_type=MESH,
        )
        handed[i].start()

    def signal(values, chunk):
        rows = []
        for k in range(outer):
            row = as_row(values[k * chunk : (k + 1) * chunk], full, tail)
            rows.append(twisted(row, twist_ref[k], full, tail) if k else row)
        return short_dft(rows)

    def backward(i):
        handed[i].wait_recv()
        chunk = sizes[i]
        both = jnp.concatenate(
            [spectrum[:, part(i), :] * keep_conj, partner[:, part(i), :] * keep_conj], axis=0
        )
        both = inner_dft(both.reshape(2 * outer * chunk, 2 * width))
        ref = signal(both[: outer * chunk], chunk)
        sec = signal(both[outer * chunk :], chunk)
        product = jnp.concatenate([times_conj(r, s).flat() for r, s in zip(ref, sec)], axis=0)
        high, low = split(product)
        weights = pool_ref[...]
        means = jnp.dot(high, weights, preferred_element_type=jnp.float32)
        means = (means + jnp.dot(low, weights, preferred_element_type=jnp.float32)) * out_scale
        looked[:, part(i), :] = means.reshape(outer, chunk, 2 * samples)
        for step in range(1, outer):
            there = lax.rem(me + step, outer)
            outgoing[i, step] = pltpu.make_async_remote_copy(
                src_ref=looked.at[there, part(i)],
                dst_ref=landed.at[rows_of(me, i)],
                send_sem=out_send.at[i, step],
                recv_sem=out_recv.at[i, step],
                device_id={"line": there},
                device_id_type=MESH,
            )
            outgoing[i, step].start()
        landed[rows_of(me, i), :] = looked[me, part(i), :]

    for i in range(chunks + 1):
        if i < chunks:
            forward(i)
        if i >= 1:
            backward(i - 1)

    for copy in outgoing.values():
        copy.wait_recv()
    out_ref[0] = landed[...].T.reshape(2, samples, columns_all)
    for copies in (incoming, handed, outgoing):
        for copy in copies.values():
            copy.wait_send()


def shards(slc, band_start, band_stop):
    outer = lax.axis_size("line")
    _, _, columns_all, width = slc.shape
    columns = columns_all // outer
    chunks = len(chunk_sizes(columns))
    samples = width // LOOKS
    inner, twist, bins, pool = (jnp.asarray(t) for t in tables(outer, width))
    vmem = pl.BlockSpec(memory_space=pltpu.VMEM)
    hbm = pl.BlockSpec(memory_space=pltpu.HBM)
    f32 = jnp.float32
    dma = pltpu.SemaphoreType.DMA
    result = pl.pallas_call(
        kernel,
        out_shape=pltpu.VMEM((1, 2, samples, columns_all), f32),
        in_specs=[hbm, hbm, hbm, hbm, hbm, hbm, hbm],
        out_specs=vmem,
        scratch_shapes=[
            pltpu.VMEM((2, width, columns_all), f32),
            pltpu.VMEM((columns_all, 2 * width), f32),
            pltpu.VMEM(inner.shape, jnp.bfloat16),
            pltpu.VMEM(twist.shape, f32),
            pltpu.VMEM(bins.shape, jnp.int32),
            pltpu.VMEM(pool.shape, jnp.bfloat16),
            pltpu.SMEM(band_start.shape, jnp.int32),
            pltpu.SMEM(band_stop.shape, jnp.int32),
            pltpu.VMEM((outer, columns, 2 * width), f32),
            pltpu.VMEM((outer, columns, 2 * width), f32),
            pltpu.VMEM((outer, columns, 2 * width), f32),
            pltpu.VMEM((outer, columns, 2 * samples), f32),
            pltpu.VMEM((columns_all, 2 * samples), f32),
            dma,
            dma((6,)),
            dma((chunks, outer)),
            dma((chunks, outer)),
            dma((chunks,)),
            dma((chunks,)),
            dma((chunks, outer)),
            dma((chunks, outer)),
        ],
        compiler_params=pltpu.CompilerParams(
            collective_id=0, has_side_effects=True, vmem_limit_bytes=66000000
        ),
    )(jnp.swapaxes(slc, 2, 3), inner, twist, bins, pool, band_start, band_stop)
    return jnp.swapaxes(result, 2, 3)


def shared_tables(outer, width):
    block = LANES // 2
    lines = outer * width
    count = lines // block
    index = np.arange(LANES) % block
    side = np.arange(LANES) // block
    angle = 2.0 * np.pi / block * (index[:, None] * index[None, :] % block)
    same = side[:, None] == side[None, :]
    dense = np.concatenate([np.where(same, np.cos(angle), 0.0), np.where(same, np.sin(angle), 0.0)], axis=1)
    dense = dense.astype(np.float32)
    high = dense.astype(jnp.bfloat16)
    low = (dense - high.astype(np.float32)).astype(jnp.bfloat16)
    inner = np.concatenate([high, high, low], axis=0)
    turn = 2.0 * np.pi / lines * (np.arange(count)[:, None] * index[None, :] % lines)
    twist = np.stack([np.cos(turn), np.sin(turn)], axis=1).astype(np.float32)
    bins = (np.arange(count)[:, None] + count * index[None, :]).astype(np.int32)[:, None, :]
    samples = width // LOOKS
    line = np.arange(width // block)[:, None, None] * block + np.arange(block)[None, None, :]
    target = line // LOOKS + samples * np.arange(2)[None, :, None]
    pool = (target.reshape(-1)[:, None] == np.arange(2 * samples)[None, :]).astype(jnp.bfloat16)
    return inner, twist, bins, pool


def turned(value, c, s):
    re, im = value
    return re * c + im * s, im * c - re * s


def plus(a, b):
    return a[0] + b[0], a[1] + b[1]


def minus(a, b):
    return a[0] - b[0], a[1] - b[1]


def times(a, factor):
    return a[0] * factor, a[1] * factor


def full_dft(values):
    count = len(values)
    if count == 1:
        return values
    if count % 2:
        sums = [plus(values[j], values[count - j]) for j in range(1, count // 2 + 1)]
        differences = [minus(values[j], values[count - j]) for j in range(1, count // 2 + 1)]
        result = [None] * count
        result[0] = functools.reduce(plus, sums, values[0])
        for k in range(1, count // 2 + 1):
            angles = [2.0 * np.pi * (j * k % count) / count for j in range(1, count // 2 + 1)]
            even = functools.reduce(plus, [times(v, float(np.cos(a))) for v, a in zip(sums, angles)], values[0])
            odd = functools.reduce(plus, [times(v, float(np.sin(a))) for v, a in zip(differences, angles)])
            result[k] = even[0] + odd[1], even[1] - odd[0]
            result[count - k] = even[0] - odd[1], even[1] + odd[0]
        return result
    even, odd = full_dft(values[0::2]), full_dft(values[1::2])
    low, high = [], []
    for k in range(count // 2):
        if k == 0:
            moved = odd[k]
        elif 4 * k == count:
            moved = odd[k][1], -odd[k][0]
        else:
            angle = 2.0 * np.pi * k / count
            moved = turned(odd[k], float(np.cos(angle)), float(np.sin(angle)))
        low.append(plus(even[k], moved))
        high.append(minus(even[k], moved))
    return low + high


def shared_kernel(
    slc_ref, inner_hbm, twist_hbm, bins_hbm, pool_hbm, start_hbm, stop_hbm, out_ref,
    raw, packed, inner, twist_ref, bins_ref, pool_ref, start_ref, stop_ref, gathered, ref_signal, sec_signal, looked, landed,
    load_sem, table_sem, in_send, in_recv, out_send, out_recv, from_below, from_above,
):
    outer = lax.axis_size("line")
    dates = lax.axis_size("date")
    me = lax.axis_index("line")
    date = lax.axis_index("date")
    width, columns_all = raw.shape[1], raw.shape[2]
    half = columns_all // 2
    rows = half // (outer * dates)
    block = LANES // 2
    blocks = width // block
    count = outer * blocks
    flat = 2 * width
    slots = slot_dates(dates)
    def at_date(relative):
        return lax.rem(date + relative, dates)

    def at_line(step):
        return lax.rem(me + step, outer)

    odd = lax.rem(date, 2)

    def slot_date(k):
        if k > 1 or dates == 2:
            return slots[k]
        return slots[k] + odd * (slots[1 - k] - slots[k])

    def device(relative, step):
        return {"date": at_date(relative), "line": at_line(step)}

    lower = me < outer // 2
    upper = me >= outer // 2
    partner = slot_date(0)

    barrier = pltpu.get_barrier_semaphore()
    for near, step in ((me > 0, outer - 1), (me < outer - 1, 1)):

        @pl.when(near)
        def _():
            for relative in (0, partner):
                pl.semaphore_signal(
                    barrier, inc=1, device_id=device(relative, step), device_id_type=MESH
                )

    for relative in range(1, dates):
        pl.semaphore_signal(barrier, inc=1, device_id=device(relative, 0), device_id_type=MESH)

    def tell(stage):
        @pl.when((me > 0) & (me + stage < outer))
        def _():
            pl.semaphore_signal(
                from_above.at[stage], inc=1, device_id={"line": me - 1}, device_id_type=MESH
            )

        @pl.when((me < outer - 1) & (me >= stage))
        def _():
            pl.semaphore_signal(
                from_below.at[stage], inc=1, device_id={"line": me + 1}, device_id_type=MESH
            )

    def hear(stage):
        @pl.when(me + stage + 1 < outer)
        def _():
            pl.semaphore_wait(from_above.at[stage], 1)

        @pl.when(me >= stage + 1)
        def _():
            pl.semaphore_wait(from_below.at[stage], 1)

    load = pltpu.make_async_copy(slc_ref.at[0], raw, load_sem)
    load.start()
    sides = (me > 0).astype(jnp.int32) + (me < outer - 1).astype(jnp.int32)
    pl.semaphore_wait(barrier, dates - 1 + 2 * sides)
    tell(0)
    tables_in = [
        pltpu.make_async_copy(source, target, table_sem.at[t])
        for t, (source, target) in enumerate(
            [
                (start_hbm, start_ref),
                (stop_hbm, stop_ref),
                (twist_hbm, twist_ref),
                (bins_hbm, bins_ref),
                (inner_hbm, inner),
                (pool_hbm, pool_ref),
            ]
        )
    ]
    load.wait()
    for table in tables_in:
        table.start()
    for part in range(2):
        for n in range(blocks):
            lines = raw[part, n * block : (n + 1) * block]
            both = jnp.concatenate([lines[:, :half], lines[:, half:]], axis=0)
            packed[:, part * flat + n * LANES : part * flat + (n + 1) * LANES] = both.T

    def rows_of(at, line):
        return pl.ds(pl.multiple_of((at * outer + line) * rows, 8), rows)

    incoming = {}
    for k in range(len(slots)):
        to = slot_date(k) if k < 2 else (dates - slots[k]) % dates
        for step in range(outer):
            if slots[k] or step:
                incoming[k, step] = pltpu.make_async_remote_copy(
                    src_ref=packed.at[rows_of(at_date(to), at_line(step))],
                    dst_ref=gathered.at[k, me],
                    send_sem=in_send.at[k, step],
                    recv_sem=in_recv.at[k, step],
                    device_id=device(to, step),
                    device_id_type=MESH,
                )

    sent = {}

    def send_in(k, step, known):
        if (k, step) not in incoming:
            return
        before = sent.get((k, step))
        sent[k, step] = known if before is None or known is None else before | known
        if before is not None:
            known = jnp.logical_not(before) if known is None else known & jnp.logical_not(before)
        if known is None:
            incoming[k, step].start()
        else:
            pl.when(known)(incoming[k, step].start)

    def distance(step):
        there = at_line(step)
        return jnp.maximum(there - me, me - there)

    def send_known(stage, ks):
        for k in ks:
            for step in range(outer - 1, -1, -1):
                near = stage + 2 if k in (0, len(slots) - 1) else stage + 1
                send_in(k, step, distance(step) <= near)

    for step, side in ((1, lower), (outer - 1, upper)):
        send_in(0, step, side)
    hear(0)
    send_known(0, [0])
    for stage in range(1, outer - 1):
        tell(stage)
        hear(stage)
    for k in range(len(slots)):
        for step in range(outer - 1, -1, -1):
            send_in(k, step, None)
    gathered[slots.index(0), me] = packed[rows_of(date, me), :]

    for table in tables_in:
        table.wait()
    bins = bins_ref[...]

    def kept(relative):
        pair = at_date(relative)
        return jnp.where((bins >= start_ref[pair]) & (bins < stop_ref[pair]), 1.0, 0.0).astype(jnp.float32)

    masks = [kept(relative) for relative in range(dates)]

    def inner_dft(re, im):
        values = jnp.concatenate([re, im], axis=0)
        high, low = split(values)
        both = jnp.dot(
            jnp.concatenate([high, low, high], axis=1), inner[...], preferred_element_type=jnp.float32
        )
        size = re.shape[0]
        return (
            both[:size, :LANES] + both[size:, LANES:],
            both[size:, :LANES] - both[:size, LANES:],
        )

    def twisted_by(values):
        return [values[0]] + [
            turned(values[n], twist_ref[n, 0:1, :], twist_ref[n, 1:2, :]) for n in range(1, len(values))
        ]

    samples = width // LOOKS
    lines_all = outer * width
    scale = 1.0 / (lines_all * lines_all * LOOKS)

    def lanes(part, n):
        return slice(part * flat + n * LANES, part * flat + (n + 1) * LANES)

    def filtered(k):
        relative = slot_date(k)
        before = (relative + dates - 1) % dates if k > 1 else lax.rem(relative + dates - 1, dates)
        values = [
            (gathered[k, l, :, lanes(0, n)], gathered[k, l, :, lanes(1, n)])
            for l in range(outer)
            for n in range(blocks)
        ]
        values = twisted_by(full_dft(values))
        re, im = inner_dft(
            jnp.concatenate([v[0] for v in values], axis=0), jnp.concatenate([v[1] for v in values], axis=0)
        )
        re, im = re.reshape(count, rows, LANES), im.reshape(count, rows, LANES)
        keeps = [masks[relative], masks[before]] if k > 1 else [kept(relative), kept(before)]
        re = jnp.concatenate([re * keep for keep in keeps], axis=0).reshape(2 * count * rows, LANES)
        im = jnp.concatenate([im * -keep for keep in keeps], axis=0).reshape(2 * count * rows, LANES)
        re, im = inner_dft(re, im)
        for base, target, pair in ((0, ref_signal, relative), (count, sec_signal, before)):
            values = [
                (re[(base + n) * rows : (base + n + 1) * rows], im[(base + n) * rows : (base + n + 1) * rows])
                for n in range(count)
            ]
            values = full_dft(twisted_by(values))
            for n, value in enumerate(values):
                for part in range(2):
                    target[pair, n // blocks, :, lanes(part, n % blocks)] = value[part]

    def multilook(pairs):
        if not pairs:
            return
        re, im = [], []
        for pair in pairs:
            for l in range(outer):
                ref_re, ref_im = ref_signal[pair, l, :, :flat], ref_signal[pair, l, :, flat:]
                sec_re, sec_im = sec_signal[pair, l, :, :flat], sec_signal[pair, l, :, flat:]
                re.append(ref_re * sec_re + ref_im * sec_im)
                im.append(ref_im * sec_re - ref_re * sec_im)
        high, low = split(jnp.concatenate(re + im, axis=0))
        means = jnp.dot(jnp.concatenate([high, low], axis=0), pool_ref[...], preferred_element_type=jnp.float32)
        size = outer * rows
        total = size * len(pairs)
        means = means[: 2 * total] + means[2 * total :]
        for n, pair in enumerate(pairs):
            re, im = means[n * size : (n + 1) * size], means[total + n * size : total + (n + 1) * size]
            looked[pair, :, :, : 2 * samples] = (re * scale).reshape(outer, rows, 2 * samples)
            looked[pair, :, :, 2 * samples :] = (im * -scale).reshape(outer, rows, 2 * samples)

    outgoing = {}

    def send_out(pair):
        for step in [*range(1, outer), 0]:
            if pair == 0 and step == 0:
                landed[rows_of(date, me), :] = looked[0, me]
                continue
            outgoing[pair, step] = pltpu.make_async_remote_copy(
                src_ref=looked.at[pair, at_line(step)],
                dst_ref=landed.at[rows_of(date, me)],
                send_sem=out_send.at[pair, step],
                recv_sem=out_recv.at[pair, step],
                device_id=device(pair, step),
                device_id_type=MESH,
            )
            outgoing[pair, step].start()

    def ready(k):
        have = slots[: k + 1]
        pairs = {slots[k], (slots[k] + dates - 1) % dates}
        return sorted((p for p in pairs if p in have and (p + 1) % dates in have), key=lambda p: p == 0)

    held = []
    for k in range(len(slots)):
        for step in range(outer):
            if (k, step) in incoming:
                incoming[k, step].wait_recv()
        final = k == len(slots) - 1
        if final:
            for pair in held:
                send_out(pair)
        filtered(k)
        multilook(ready(k))
        for pair in ready(k):
            if final:
                send_out(pair)
            else:
                held.append(pair)

    for copy in outgoing.values():
        copy.wait_recv()
    for part in range(2):
        turned_back = landed[:, part * 2 * samples : (part + 1) * 2 * samples].T
        out_ref[0, part, :, :half] = turned_back[:samples]
        out_ref[0, part, :, half:] = turned_back[samples:]
    for copies in (incoming, outgoing):
        for copy in copies.values():
            copy.wait_send()


def slot_dates(dates):
    return list(range(1, dates, 2)) + list(range(2, dates, 2)) + [0]


def shared_shards(slc, band_start, band_stop):
    outer = lax.axis_size("line")
    dates = lax.axis_size("date")
    _, _, columns_all, width = slc.shape
    half = columns_all // 2
    rows = half // (outer * dates)
    samples = width // LOOKS
    inner, twist, bins, pool = (jnp.asarray(t) for t in shared_tables(outer, width))
    vmem = pl.BlockSpec(memory_space=pltpu.VMEM)
    hbm = pl.BlockSpec(memory_space=pltpu.HBM)
    f32 = jnp.float32
    dma = pltpu.SemaphoreType.DMA
    result = pl.pallas_call(
        shared_kernel,
        out_shape=pltpu.VMEM((1, 2, samples, columns_all), f32),
        in_specs=[hbm, hbm, hbm, hbm, hbm, hbm, hbm],
        out_specs=vmem,
        scratch_shapes=[
            pltpu.VMEM((2, width, columns_all), f32),
            pltpu.VMEM((half, 4 * width), f32),
            pltpu.VMEM(inner.shape, jnp.bfloat16),
            pltpu.VMEM(twist.shape, f32),
            pltpu.VMEM(bins.shape, jnp.int32),
            pltpu.VMEM(pool.shape, jnp.bfloat16),
            pltpu.SMEM(band_start.shape, jnp.int32),
            pltpu.SMEM(band_stop.shape, jnp.int32),
            pltpu.VMEM((dates, outer, rows, 4 * width), f32),
            pltpu.VMEM((dates, outer, rows, 4 * width), f32),
            pltpu.VMEM((dates, outer, rows, 4 * width), f32),
            pltpu.VMEM((dates, outer, rows, 4 * samples), f32),
            pltpu.VMEM((half, 4 * samples), f32),
            dma,
            dma((6,)),
            dma((dates, outer)),
            dma((dates, outer)),
            dma((dates, outer)),
            dma((dates, outer)),
            pltpu.SemaphoreType.REGULAR((outer,)),
            pltpu.SemaphoreType.REGULAR((outer,)),
        ],
        compiler_params=pltpu.CompilerParams(
            collective_id=0, has_side_effects=True, vmem_limit_bytes=66000000
        ),
    )(jnp.swapaxes(slc, 2, 3), inner, twist, bins, pool, band_start, band_stop)
    return jnp.swapaxes(result, 2, 3)


def solution(mesh):
    group = mesh.shape["line"] * mesh.shape["date"]

    def body(slc, band_start, band_stop):
        half, width = slc.shape[2] // 2, slc.shape[3]
        shared = half % (8 * group) == 0 and half % LANES == 0 and mesh.shape["date"] % 2 == 0
        shared = shared and width % LANES == LANES // 2 and 2 * (width // LOOKS) % LANES == 0
        return (shared_shards if shared else shards)(slc, band_start, band_stop)

    return jax.shard_map(
        body,
        mesh=mesh,
        in_specs=(P("date", None, "stack", "line"), P(), P()),
        out_specs=P("date", None, "stack", "line"),
        check_vma=False,
    )
```
